64 devices in a mesh: rep: 8 (over x, y, core), dp: 8 (over z).
Axes of the slice: x: 2, y: 2, z: 8, core: 2. Of those that a mesh axis runs over, the one named last changes fastest.
The devices are a block of a 4x4x8 slice.
Arguments:
- g_w_gate: bfloat16 [64, 2, 512, 1408], P(('rep', 'dp')), parts along dimension 0
- g_w_up: bfloat16 [64, 2, 512, 1408], P(('rep', 'dp')), parts along dimension 0
- g_w_down: bfloat16 [64, 2, 1408, 512], P(('rep', 'dp')), parts along dimension 0
- w_gate: bfloat16 [2, 512, 1408], replicated
- w_up: bfloat16 [2, 512, 1408], replicated
- w_down: bfloat16 [2, 1408, 512], replicated
- m_w_gate: float32 [2, 512, 1408], P(None, 'dp')
- m_w_up: float32 [2, 512, 1408], P(None, 'dp')
- m_w_down: float32 [2, 1408, 512], P(None, 'dp')
- v_w_gate: float32 [2, 512, 1408], P(None, 'dp')
- v_w_up: float32 [2, 512, 1408], P(None, 'dp')
- v_w_down: float32 [2, 1408, 512], P(None, 'dp')
Outputs:
- output 1: bfloat16 [16, 512, 1408], P('rep'), parts along dimension 0
- output 2: bfloat16 [16, 512, 1408], P('rep'), parts along dimension 0
- output 3: bfloat16 [16, 1408, 512], P('rep'), parts along dimension 0
- output 4: float32 [16, 512, 1408], P('rep', 'dp'), parts along dimension 0
- output 5: float32 [16, 512, 1408], P('rep', 'dp'), parts along dimension 0
- output 6: float32 [16, 1408, 512], P('rep', 'dp'), parts along dimension 0
- output 7: float32 [16, 512, 1408], P('rep', 'dp'), parts along dimension 0
- output 8: float32 [16, 512, 1408], P('rep', 'dp'), parts along dimension 0
- output 9: float32 [16, 1408, 512], P('rep', 'dp'), parts along dimension 0
There are 8 independent parts. The reference program is written for one: setup_inputs(seed, part) draws one part's arguments, and reference() takes and returns one part's arrays. A program takes and returns all parts, laid end to end along the dimension named above; an argument that names none is the same for every part.
All inputs are finite; a program needn't handle non-finite values.
Results may differ from the reference program's by a relative error of at most 0.022.
Values are sent between devices in bfloat16 or wider.
A program may use at most 768 MiB of HBM per device.

```python
import jax
import jax.numpy as jnp
from jax import lax

DEVICES = 8
D = 512
FF = 1408
LAYERS = 2
NAMES = ("w_gate", "w_up", "w_down")
SHAPES = {"w_gate": (LAYERS, D, FF), "w_up": (LAYERS, D, FF), "w_down": (LAYERS, FF, D)}


def setup_inputs(seed: int = 0, part: int = 0) -> dict:
    kz, *keys = jax.random.split(jax.random.key(seed), 1 + 5 * len(NAMES))
    loud = 2.0 ** jax.random.uniform(kz, (), jnp.float32, -1.0, 1.0)
    drawn = {}
    for name, key, both in zip(NAMES, keys[:3], keys[3:6], strict=True):
        own = jax.random.normal(jax.random.fold_in(key, part), (DEVICES, *SHAPES[name]), jnp.float32)
        shared = jax.random.normal(jax.random.fold_in(both, part), SHAPES[name], jnp.float32)
        drawn["g_" + name] = (loud * (0.7 * shared / DEVICES + 0.7 * own * DEVICES**-0.5)).astype(jnp.bfloat16)
    for name, key in zip(NAMES, keys[6:9], strict=True):
        drawn[name] = (jax.random.normal(key, SHAPES[name], jnp.float32) * SHAPES[name][1] ** -0.5).astype(jnp.bfloat16)
    for name, key in zip(NAMES, keys[9:12], strict=True):
        drawn["m_" + name] = loud * 0.5 * jax.random.normal(key, SHAPES[name], jnp.float32)
    for name, key in zip(NAMES, keys[12:15], strict=True):
        drawn["v_" + name] = loud * loud * jax.random.uniform(key, SHAPES[name], jnp.float32, 0.5, 1.5)
    return drawn


def adamw(w, m, v, g):
    m = 0.9 * m + 0.1 * g
    v = 0.95 * v + 0.05 * g * g
    step = m * lax.rsqrt(v + 1e-8) + 0.1 * w
    return (w - 0.02 * step).astype(jnp.bfloat16), m, v


def clipped(gradients, sum_of_squares, count):
    factor = jnp.minimum(1.0, 0.5 * lax.rsqrt(sum_of_squares / count + 1e-30))
    return [g * factor for g in gradients]


def reference(g_w_gate, g_w_up, g_w_down, w_gate, w_up, w_down, m_w_gate, m_w_up, m_w_down, v_w_gate, v_w_up, v_w_down):
    def total(terms):
        return lax.scan(lambda so_far, term: (so_far + term.astype(jnp.float32), None), jnp.zeros(terms.shape[1:], jnp.float32), terms)[0]

    gradients = [total(terms).astype(jnp.bfloat16).astype(jnp.float32) for terms in (g_w_gate, g_w_up, g_w_down)]
    gradients = clipped(gradients, sum(jnp.sum(g * g) for g in gradients), sum(g.size for g in gradients))
    new = [
        adamw(w.astype(jnp.float32), m, v, g)
        for w, m, v, g in zip((w_gate, w_up, w_down), (m_w_gate, m_w_up, m_w_down), (v_w_gate, v_w_up, v_w_down), gradients, strict=True)
    ]
    return tuple(one[which] for which in range(3) for one in new)
```

```python
import functools

import jax
import jax.numpy as jnp
from jax import lax
from jax.experimental import pallas as pl
from jax.experimental.pallas import tpu as pltpu
from jax.sharding import PartitionSpec as P

MESH = pl.DeviceIdType.MESH
TILE = 16


def adamw(w, m, v, g):
    m = 0.9 * m + 0.1 * g
    v = 0.95 * v + 0.05 * g * g
    step = m * lax.rsqrt(v + 1e-8) + 0.1 * w
    return (w - 0.02 * step).astype(jnp.bfloat16), m, v


def kernel(n, count, *refs):
    terms, weights, m_in, v_in = (refs[i : i + 3] for i in (0, 3, 6, 9))
    w_out, m_out, v_out = (refs[i : i + 3] for i in (12, 15, 18))
    held, came, own, m_own, v_own, total = (refs[i : i + 3] for i in (21, 24, 27, 30, 33, 36))
    parts, load_sem, own_sem, send_sem, recv_sem, part_send, part_recv = refs[39:]
    me = lax.axis_index("dp")
    right, left = lax.rem(me + 1, n), lax.rem(me + n - 1, n)
    rows = [m.shape[1] for m in m_in]
    half = n // 2
    towards = (right, left)
    hops = [[half - (layer != way) for layer in range(2)] for way in range(2)]

    def at(away):
        return lax.rem(me + away + n, n)

    def block(ref, k, layer, who):
        return ref.at[layer, pl.ds(pl.multiple_of(who * rows[k], rows[k]), rows[k])]

    def sign(way, away):
        return away if way == 0 else -away

    order = []
    for s in range(half + 1):
        for way in range(2):
            for layer in (way, 1 - way):
                j = sign(way, hops[way][layer] - s) % n
                if hops[way][layer] - s >= 0 and (layer, j) not in order:
                    order.append((layer, j))
    loads = {}
    for layer, j in order:
        for k in range(3):
            loads[layer, j, k] = pltpu.make_async_copy(
                block(terms[k].at[0], k, layer, at(j)), held[k].at[layer, j], load_sem.at[layer, j, k]
            )
            loads[layer, j, k].start()
    owns = []
    for k in range(3):
        owns += [
            pltpu.make_async_copy(weights[k].at[:, pl.ds(pl.multiple_of(me * rows[k], rows[k]), rows[k])], own[k], own_sem.at[0, k]),
            pltpu.make_async_copy(m_in[k], m_own[k], own_sem.at[1, k]),
            pltpu.make_async_copy(v_in[k], v_own[k], own_sem.at[2, k]),
        ]

    barrier = pltpu.get_barrier_semaphore()
    for peer in towards:
        pl.semaphore_signal(barrier, inc=1, device_id={"dp": peer}, device_id_type=MESH)
    pl.semaphore_wait(barrier, 2)

    def sum_copy(way, layer, s, k):
        slot = 2 * s + (layer != way)
        source = held[k].at[layer, sign(way, hops[way][layer]) % n] if s == 0 else came[k].at[way, 2 * (s - 1) + (layer != way)]
        return pltpu.make_async_remote_copy(
            src_ref=source,
            dst_ref=came[k].at[way, slot],
            send_sem=send_sem.at[way, slot, k],
            recv_sem=recv_sem.at[way, slot, k],
            device_id={"dp": towards[way]},
            device_id_type=MESH,
        )

    for which in range(2):
        for k in range(3):
            for way in range(2):
                layer = way if which == 0 else 1 - way
                loads[layer, sign(way, hops[way][layer]) % n, k].wait()
                sum_copy(way, layer, 0, k).start()
    for copy in owns:
        copy.start()

    squares = jnp.zeros((8, 128), jnp.float32)
    for s in range(half):
        for which in range(2):
            for k in range(3):
                for way in range(2):
                    layer = way if which == 0 else 1 - way
                    here = hops[way][layer] - 1 - s
                    if here < 0:
                        continue
                    slot = 2 * s + which
                    mine = came[k].at[way, slot]
                    sum_copy(way, layer, s, k).wait_recv()
                    if here > 0:
                        j = sign(way, here) % n
                        loads[layer, j, k].wait()
                        term = held[k].at[layer, j]

                        @pl.loop(0, rows[k] // TILE)
                        def _(t):
                            tile = pl.ds(pl.multiple_of(t * TILE, TILE), TILE)
                            mine[tile] = (mine[tile].astype(jnp.float32) + term[tile].astype(jnp.float32)).astype(jnp.bfloat16)

                        sum_copy(way, layer, s + 1, k).start()
                    elif which == 0:
                        other = came[k].at[1 - way, 2 * (s - 1) + 1]
                        loads[layer, 0, k].wait()
                        term, to = held[k].at[layer, 0], total[k].at[layer]

                        def add(t, squares):
                            tile = pl.ds(pl.multiple_of(t * TILE, TILE), TILE)
                            g = term[tile].astype(jnp.float32) + mine[tile].astype(jnp.float32) + other[tile].astype(jnp.float32)
                            g = g.astype(jnp.bfloat16)
                            to[tile] = g
                            g = g.astype(jnp.float32)
                            return squares + jnp.sum((g * g).reshape(-1, 8, to.shape[-1] // 128, 128), axis=(0, 2))

                        squares = lax.fori_loop(0, rows[k] // TILE, add, squares)

    parts[me] = squares
    for away in range(1, n):
        pltpu.make_async_remote_copy(
            src_ref=parts.at[me],
            dst_ref=parts.at[me],
            send_sem=part_send.at[away],
            recv_sem=part_recv.at[me],
            device_id={"dp": at(away)},
            device_id_type=MESH,
        ).start()
    for copy in owns:
        copy.wait()
    for way in range(2):
        for layer in range(2):
            for s in range(hops[way][layer]):
                for k in range(3):
                    sum_copy(way, layer, s, k).wait_send()
    for away in range(1, n):
        pltpu.make_async_remote_copy(
            src_ref=parts.at[at(away)],
            dst_ref=parts.at[at(away)],
            send_sem=part_send.at[away],
            recv_sem=part_recv.at[at(away)],
            device_id={"dp": at(away)},
            device_id_type=MESH,
        ).wait()
    everything = parts[0]
    for i in range(1, n):
        everything = everything + parts[i]
    factor = jnp.minimum(1.0, 0.5 * lax.rsqrt(jnp.sum(everything, keepdims=True) / count + 1e-30))

    def weight_copy(way, layer, s, k):
        ref = block(w_out[k], k, layer, at(-sign(way, s)))
        slot = 2 * s + (layer != way)
        return pltpu.make_async_remote_copy(
            src_ref=ref,
            dst_ref=ref,
            send_sem=send_sem.at[way, slot, k],
            recv_sem=recv_sem.at[way, slot, k],
            device_id={"dp": towards[way]},
            device_id_type=MESH,
        )

    for k in range(3):
        for layer in range(2):
            to = block(w_out[k], k, layer, me)

            @pl.loop(0, rows[k] // TILE)
            def _(t):
                tile = pl.ds(pl.multiple_of(t * TILE, TILE), TILE)
                g = total[k][layer, tile].astype(jnp.float32) * factor
                w, m, v = adamw(own[k][layer, tile].astype(jnp.float32), m_own[k][layer, tile], v_own[k][layer, tile], g)
                to[tile] = w
                m_out[k][layer, tile] = m
                v_out[k][layer, tile] = v

            for way in range(2):
                weight_copy(way, layer, 0, k).start()
    for s in range(half):
        for k in range(3):
            for layer in range(2):
                for way in range(2):
                    if s >= hops[way][layer]:
                        continue
                    slot = 2 * s + (layer != way)
                    ref = block(w_out[k], k, layer, at(-sign(way, s + 1)))
                    pltpu.make_async_remote_copy(
                        src_ref=ref,
                        dst_ref=ref,
                        send_sem=send_sem.at[way, slot, k],
                        recv_sem=recv_sem.at[way, slot, k],
                        device_id={"dp": towards[way]},
                        device_id_type=MESH,
                    ).wait_recv()
                    if s + 1 < hops[way][layer]:
                        weight_copy(way, layer, s + 1, k).start()
    for way in range(2):
        for layer in range(2):
            for s in range(hops[way][layer]):
                for k in range(3):
                    weight_copy(way, layer, s, k).wait_send()


def flush(*refs):
    sem = refs[-1]
    half = len(refs) // 2
    copies = [pltpu.make_async_copy(refs[i], refs[half + i], sem.at[i]) for i in range(half)]
    for copy in copies:
        copy.start()
    for copy in copies:
        copy.wait()


def solution(mesh):
    def step(*arrays):
        n = lax.axis_size("dp")
        terms, weights, m, v = (arrays[i : i + 3] for i in (0, 3, 6, 9))
        count = sum(w.size for w in weights)
        shapes = [(w.shape, w.dtype) for w in weights] + [(x.shape, x.dtype) for x in (*m, *v)]
        blocks = [(one.shape[1], one.shape[2]) for one in m]
        half = n // 2
        outs = pl.pallas_call(
            functools.partial(kernel, n, count),
            name="step",
            out_shape=[pltpu.VMEM(s, d) for s, d in shapes],
            in_specs=[pl.BlockSpec(memory_space=pl.ANY)] * 12,
            out_specs=[pl.BlockSpec(memory_space=pltpu.VMEM)] * 9,
            scratch_shapes=[
                *(pltpu.VMEM((2, n, *b), jnp.bfloat16) for b in blocks),
                *(pltpu.VMEM((2, 2 * half - 1, *b), jnp.bfloat16) for b in blocks),
                *(pltpu.VMEM((2, *b), jnp.bfloat16) for b in blocks),
                *(pltpu.VMEM((2, *b), jnp.float32) for b in blocks),
                *(pltpu.VMEM((2, *b), jnp.float32) for b in blocks),
                *(pltpu.VMEM((2, *b), jnp.bfloat16) for b in blocks),
                pltpu.VMEM((n, 8, 128), jnp.float32),
                pltpu.SemaphoreType.DMA((2, n, 3)),
                pltpu.SemaphoreType.DMA((3, 3)),
                pltpu.SemaphoreType.DMA((2, 2 * half - 1, 3)),
                pltpu.SemaphoreType.DMA((2, 2 * half - 1, 3)),
                pltpu.SemaphoreType.DMA((n,)),
                pltpu.SemaphoreType.DMA((n,)),
            ],
            compiler_params=pltpu.CompilerParams(collective_id=0, has_side_effects=True, vmem_limit_bytes=44 * 2**20),
        )(*arrays)
        return tuple(outs)

    all_of, cut = P(None, None, None), P(None, "dp", None)
    return jax.shard_map(
        step,
        mesh=mesh,
        in_specs=(P(("rep", "dp"), None, None, None),) * 3 + (all_of,) * 3 + (cut,) * 6,
        out_specs=(P("rep", None, None),) * 3 + (P("rep", "dp", None),) * 6,
        check_vma=False,
    )
```

```python
import functools

import jax
import jax.numpy as jnp
from jax import lax
from jax.experimental import pallas as pl
from jax.experimental.pallas import tpu as pltpu
from jax.sharding import PartitionSpec as P

MESH = pl.DeviceIdType.MESH
TILE = 16


def adamw(w, m, v, g):
    m = 0.9 * m + 0.1 * g
    v = 0.95 * v + 0.05 * g * g
    step = m * lax.rsqrt(v + 1e-8) + 0.1 * w
    return (w - 0.02 * step).astype(jnp.bfloat16), m, v


def pieces(rows):
    head, tail = TILE, 2 * TILE
    return [(0, 0, head), (0, head, rows[0] - head), (1, 0, rows[1]), (2, 0, rows[2] - tail), (2, rows[2] - tail, tail)]


def kernel(n, count, *refs):
    terms, weights, m_in, v_in = (refs[i : i + 3] for i in (0, 3, 6, 9))
    w_out, m_out, v_out = (refs[i : i + 3] for i in (12, 15, 18))
    held, came, own, m_own, v_own, total = (refs[i : i + 3] for i in (21, 24, 27, 30, 33, 36))
    parts, load_sem, own_sem, send_sem, recv_sem, part_send, part_recv = refs[39:]
    me = lax.axis_index("dp")
    rows = [m.shape[1] for m in m_in]
    cuts = pieces(rows)
    half = n // 2

    def at(away):
        return lax.rem(me + away + n, n)

    towards = (at(1), at(-1))
    hops = [[half - (layer != way) for layer in range(2)] for way in range(2)]

    barrier = pltpu.get_barrier_semaphore()
    for peer in towards:
        pl.semaphore_signal(barrier, inc=1, device_id={"dp": peer}, device_id_type=MESH)

    def block(ref, layer, who, k, first=0, size=None):
        return ref.at[layer, pl.ds(pl.multiple_of(who * rows[k] + first, TILE), size or rows[k])]

    def sign(way, away):
        return away if way == 0 else -away

    order = [(way, sign(way, half) % n) for way in range(2)] + [(1 - way, sign(way, half - 1) % n) for way in range(2)]
    order = list(dict.fromkeys(order))
    for j in [j for d in range(half - 1, -1, -1) for j in (d, n - d)]:
        for layer in range(2):
            if (layer, j % n) not in order:
                order.append((layer, j % n))
    loads = {
        (layer, j, k): pltpu.make_async_copy(block(terms[k].at[0], layer, at(j), k), held[k].at[layer, j], load_sem.at[layer, j, k])
        for layer, j in order
        for k in range(3)
    }
    owns = []
    for k in range(3):
        owns += [
            pltpu.make_async_copy(weights[k].at[:, pl.ds(pl.multiple_of(me * rows[k], rows[k]), rows[k])], own[k], own_sem.at[0, k]),
            pltpu.make_async_copy(m_in[k], m_own[k], own_sem.at[1, k]),
            pltpu.make_async_copy(v_in[k], v_own[k], own_sem.at[2, k]),
        ]
    first = [(layer, j, k) for layer, j in order[:4] for k in range(3)]
    for key in first:
        loads[key].start()
    with jax.named_scope("barrier"):
        pl.semaphore_wait(barrier, 2)

    def sum_copy(way, layer, s, p):
        k, start, size = cuts[p]
        slot = 2 * s + (layer != way)
        source = held[k].at[layer, sign(way, hops[way][layer]) % n] if s == 0 else came[k].at[way, 2 * (s - 1) + (layer != way)]
        return pltpu.make_async_remote_copy(
            src_ref=source.at[pl.ds(start, size)],
            dst_ref=came[k].at[way, slot, pl.ds(start, size)],
            send_sem=send_sem.at[way, slot, p],
            recv_sem=recv_sem.at[way, slot, p],
            device_id={"dp": towards[way]},
            device_id_type=MESH,
        )

    waited = set()
    def loaded(*key):
        if key not in waited:
            waited.add(key)
            loads[key].wait()

    with jax.named_scope("first"):
        for which in range(2):
            for p, (k, _, _) in enumerate(cuts):
                for way in range(2):
                    layer = way if which == 0 else 1 - way
                    loaded(layer, sign(way, hops[way][layer]) % n, k)
                    sum_copy(way, layer, 0, p).start()
        for key, copy in loads.items():
            if key not in first:
                copy.start()
        for copy in owns:
            copy.start()

    squares = jnp.zeros((8, 128), jnp.float32)
    for s in range(half):
        for which in range(2):
            for p, (k, start, size) in enumerate(cuts):
                for way in range(2):
                    layer = way if which == 0 else 1 - way
                    here = hops[way][layer] - 1 - s
                    if here < 0:
                        continue
                    slot = 2 * s + which
                    mine = came[k].at[way, slot]
                    with jax.named_scope(f"recv{s}{which}{p}{way}"):
                        sum_copy(way, layer, s, p).wait_recv()
                    if here > 0:
                        j = sign(way, here) % n
                        loaded(layer, j, k)
                        term = held[k].at[layer, j]

                        @pl.loop(0, size // TILE)
                        def _(t):
                            tile = pl.ds(pl.multiple_of(start + t * TILE, TILE), TILE)
                            mine[tile] = (mine[tile].astype(jnp.float32) + term[tile].astype(jnp.float32)).astype(jnp.bfloat16)

                        sum_copy(way, layer, s + 1, p).start()
                    elif which == 0:
                        other = came[k].at[1 - way, 2 * (s - 1) + 1]
                        loaded(layer, 0, k)
                        term, to = held[k].at[layer, 0], total[k].at[layer]

                        def add(t, squares):
                            tile = pl.ds(pl.multiple_of(start + t * TILE, TILE), TILE)
                            g = term[tile].astype(jnp.float32) + mine[tile].astype(jnp.float32) + other[tile].astype(jnp.float32)
                            g = g.astype(jnp.bfloat16)
                            to[tile] = g
                            g = g.astype(jnp.float32)
                            g = g * g
                            for i in range(TILE // 8):
                                for c in range(g.shape[1] // 128):
                                    squares = squares + g[8 * i : 8 * i + 8, 128 * c : 128 * c + 128]
                            return squares

                        squares = lax.fori_loop(0, size // TILE, add, squares)

    def part_copy(away, sender):
        ref = parts.at[pl.ds(sender, 1)]
        return pltpu.make_async_remote_copy(
            src_ref=ref,
            dst_ref=ref,
            send_sem=part_send.at[away % n],
            recv_sem=part_recv.at[sender],
            device_id={"dp": at(away)},
            device_id_type=MESH,
        )

    far = sorted(range(1, n), key=lambda away: -min(away, n - away))
    with jax.named_scope("exchange"):
        parts[pl.ds(me, 1)] = jnp.sum(squares, axis=0, keepdims=True)
        for away in far:
            part_copy(away, me).start()
        for copy in owns:
            copy.wait()
        for way in range(2):
            for layer in range(2):
                for s in range(hops[way][layer]):
                    for p in range(len(cuts)):
                        sum_copy(way, layer, s, p).wait_send()
        for away in far[::-1]:
            part_copy(away, at(away)).wait()
    factor = jnp.minimum(1.0, 0.5 * lax.rsqrt(jnp.sum(parts[...], keepdims=True) / count + 1e-30))

    def weight_copy(way, layer, s, p, sender):
        k, start, size = cuts[p]
        ref = block(w_out[k], layer, sender, k, start, size)
        slot = 2 * s + (layer != way)
        return pltpu.make_async_remote_copy(
            src_ref=ref,
            dst_ref=ref,
            send_sem=send_sem.at[way, slot, p],
            recv_sem=recv_sem.at[way, slot, p],
            device_id={"dp": towards[way]},
            device_id_type=MESH,
        )

    for p, (k, start, size) in enumerate(cuts):
        for layer in range(2):
            to = block(w_out[k], layer, me, k)

            with jax.named_scope(f"adamw{p}{layer}"):

                @pl.loop(0, size // TILE)
                def _(t):
                    tile = pl.ds(pl.multiple_of(start + t * TILE, TILE), TILE)
                    g = total[k][layer, tile].astype(jnp.float32) * factor
                    w, m, v = adamw(own[k][layer, tile].astype(jnp.float32), m_own[k][layer, tile], v_own[k][layer, tile], g)
                    to[tile] = w
                    m_out[k][layer, tile] = m
                    v_out[k][layer, tile] = v

            for way in range(2):
                weight_copy(way, layer, 0, p, me).start()
    for s in range(half):
        for p in range(len(cuts)):
            for layer in range(2):
                for way in range(2):
                    if s >= hops[way][layer]:
                        continue
                    with jax.named_scope(f"get{s}{p}{layer}{way}"):
                        weight_copy(way, layer, s, p, at(-sign(way, s + 1))).wait_recv()
                    if s + 1 < hops[way][layer]:
                        weight_copy(way, layer, s + 1, p, at(-sign(way, s + 1))).start()
    with jax.named_scope("ends"):
        for way in range(2):
            for layer in range(2):
                for s in range(hops[way][layer]):
                    for p in range(len(cuts)):
                        weight_copy(way, layer, s, p, at(-sign(way, s))).wait_send()


def flush(*refs):
    sem = refs[-1]
    half = len(refs) // 2
    copies = [pltpu.make_async_copy(refs[i], refs[half + i], sem.at[i]) for i in range(half)]
    for copy in copies:
        copy.start()
    for copy in copies:
        copy.wait()


def solution(mesh):
    def step(*arrays):
        n = lax.axis_size("dp")
        terms, weights, m, v = (arrays[i : i + 3] for i in (0, 3, 6, 9))
        count = sum(w.size for w in weights)
        shapes = [(w.shape, w.dtype) for w in weights] + [(x.shape, x.dtype) for x in (*m, *v)]
        blocks = [(one.shape[1], one.shape[2]) for one in m]
        half, cuts = n // 2, len(pieces([b[0] for b in blocks]))
        outs = pl.pallas_call(
            functools.partial(kernel, n, count),
            name="step",
            out_shape=[pltpu.VMEM(s, d) for s, d in shapes],
            in_specs=[pl.BlockSpec(memory_space=pl.ANY)] * 12,
            out_specs=[pl.BlockSpec(memory_space=pltpu.VMEM)] * 9,
            scratch_shapes=[
                *(pltpu.VMEM((2, n, *b), jnp.bfloat16) for b in blocks),
                *(pltpu.VMEM((2, 2 * half - 1, *b), jnp.bfloat16) for b in blocks),
                *(pltpu.VMEM((2, *b), jnp.bfloat16) for b in blocks),
                *(pltpu.VMEM((2, *b), jnp.float32) for b in blocks),
                *(pltpu.VMEM((2, *b), jnp.float32) for b in blocks),
                *(pltpu.VMEM((2, *b), jnp.bfloat16) for b in blocks),
                pltpu.VMEM((n, 128), jnp.float32),
                pltpu.SemaphoreType.DMA((2, n, 3)),
                pltpu.SemaphoreType.DMA((3, 3)),
                pltpu.SemaphoreType.DMA((2, 2 * half - 1, cuts)),
                pltpu.SemaphoreType.DMA((2, 2 * half - 1, cuts)),
                pltpu.SemaphoreType.DMA((n,)),
                pltpu.SemaphoreType.DMA((n,)),
            ],
            compiler_params=pltpu.CompilerParams(collective_id=0, has_side_effects=True, vmem_limit_bytes=44 * 2**20),
        )(*arrays)
        return tuple(
            pl.pallas_call(
                flush,
                name="flush",
                out_shape=[jax.ShapeDtypeStruct(s, d) for s, d in shapes],
                in_specs=[pl.BlockSpec(memory_space=pltpu.VMEM)] * 9,
                out_specs=[pl.BlockSpec(memory_space=pl.ANY)] * 9,
                scratch_shapes=[pltpu.SemaphoreType.DMA((9,))],
                compiler_params=pltpu.CompilerParams(vmem_limit_bytes=2**20),
            )(*outs)
        )

    all_of, cut = P(None, None, None), P(None, "dp", None)
    return jax.shard_map(
        step,
        mesh=mesh,
        in_specs=(P(("rep", "dp"), None, None, None),) * 3 + (all_of,) * 3 + (cut,) * 6,
        out_specs=(P("rep", None, None),) * 3 + (P("rep", "dp", None),) * 6,
        check_vma=False,
    )
```

```python
import functools

import jax
import jax.numpy as jnp
from jax import lax
from jax.experimental import pallas as pl
from jax.experimental.pallas import tpu as pltpu
from jax.sharding import PartitionSpec as P

MESH = pl.DeviceIdType.MESH
TILE = 16
LATER = 13500


def adamw(w, m, v, g):
    m = 0.9 * m + 0.1 * g
    v = 0.95 * v + 0.05 * g * g
    step = m * lax.rsqrt(v + 1e-8) + 0.1 * w
    return (w - 0.02 * step).astype(jnp.bfloat16), m, v


class Gather:
    def __init__(self, n, towards, layers, hops, send_sem, recv_sem):
        self.n, self.towards, self.layers, self.hops = n, towards, layers, hops
        self.send_sem, self.recv_sem = send_sem, recv_sem
        self.me = lax.axis_index("dp")

    def behind(self, way, s):
        return lax.rem(self.me + (-s if way == 0 else s) + self.n, self.n)

    def copy(self, ref, way, short, s, p, sender, rows, start=0, size=None, source=None):
        to = ref.at[self.layers[way][short], pl.ds(pl.multiple_of(sender * rows + start, TILE), size or rows)]
        return pltpu.make_async_remote_copy(
            src_ref=to if source is None else source,
            dst_ref=to,
            send_sem=self.send_sem.at[way, short, p],
            recv_sem=self.recv_sem.at[way, 2 * s + short, p],
            device_id={"dp": self.towards[way]},
            device_id_type=MESH,
        )

    def forward(self, pieces, own=None):
        for s in range(self.hops[0]):
            for p, (ref, *piece) in enumerate(pieces):
                rows, start, size = piece
                for short in range(2):
                    for way in range(2):
                        if s >= self.hops[short]:
                            continue

                        def copy(step, behind, source=None):
                            return self.copy(ref, way, short, step, p, self.behind(way, behind), rows, start, size, source)

                        with jax.named_scope(f"get{s}{p}{short}{way}"):
                            copy(s, s + 1).wait_recv()
                        mine = own.at[self.layers[way][short], pl.ds(start, size)] if own is not None and s == 0 else None
                        copy(s, s, mine).wait_send()
                        if s + 1 < self.hops[short]:
                            copy(s + 1, s + 1).start()


def kernel(n, count, *refs):
    terms, weights, m_in, v_in = (refs[i : i + 3] for i in (0, 3, 6, 9))
    w_out, m_out, v_out = (refs[i : i + 3] for i in (12, 15, 18))
    raw, held, came, own, m_own, v_own, total = (refs[i : i + 3] for i in range(21, 42, 3))
    parts, load_sem, own_sem, send_sem, recv_sem, part_sem = refs[42:]
    me = lax.axis_index("dp")
    rows = [m.shape[1] for m in m_in]
    half = n // 2

    def at(away):
        return lax.rem(me + away + n, n)

    def sign(way, away):
        return away if way == 0 else -away

    def block(ref, layer, who, k):
        return ref.at[layer, pl.ds(pl.multiple_of(who * rows[k], rows[k]), rows[k])]

    towards = (at(1), at(-1))
    layers = [[way, 1 - way] for way in range(2)]
    hops = [half, half - 1]

    barrier = pltpu.get_barrier_semaphore()
    for peer in towards:
        pl.semaphore_signal(barrier, inc=1, device_id={"dp": peer}, device_id_type=MESH)

    def first(way, short, k, sem):
        source = block(terms[k].at[0], layers[way][short], at(sign(way, hops[short])), k)
        return pltpu.make_async_copy(source, raw[k].at[way, short], load_sem.at[sem])

    rest = [pltpu.make_async_copy(terms[k].at[0], held[k], load_sem.at[k]) for k in range(3)]
    owns = [
        pltpu.make_async_copy(source, to, own_sem.at[i, k])
        for k in range(3)
        for i, (source, to) in enumerate(
            [(weights[k].at[:, pl.ds(pl.multiple_of(me * rows[k], rows[k]), rows[k])], own[k]), (m_in[k], m_own[k]), (v_in[k], v_own[k])]
        )
    ]
    for way in range(2):
        first(way, 0, 0, 3).start()
    pl.semaphore_wait(barrier, 2)
    for k in range(3):
        for short in range(k == 0, 2):
            for way in range(2):
                first(way, short, k, k).start()

    @pl.when(lax.rem(lax.axis_index("rep"), 2) == 1)
    def _():
        pl.delay(LATER)

    def send(way, short, s, k, source, to):
        return pltpu.make_async_remote_copy(
            src_ref=source,
            dst_ref=to,
            send_sem=send_sem.at[way, short, k],
            recv_sem=recv_sem.at[way, 2 * s + short, k],
            device_id={"dp": towards[way]},
            device_id_type=MESH,
        )

    def sum_copy(way, short, s, k):
        source = raw[k].at[way, short] if s == 0 else came[k].at[way, 2 * (s - 1) + short]
        return send(way, short, s, k, source, came[k].at[way, 2 * s + short])

    with jax.named_scope("first"):
        for k in range(3):
            for short in range(2):
                if k == 0 or not short:
                    ready = raw[k] if k else raw[k].at[:, short]
                    pltpu.make_async_copy(ready, ready, load_sem.at[0 if short else (3, 1, 2)[k]]).wait()
                for way in range(2):
                    sum_copy(way, short, 0, k).start()
            rest[k].start()
        for copy in owns:
            copy.start()

    squares = jnp.zeros((8, 128), jnp.float32)
    waited = set()
    for s in range(half):
        for k in range(3):
            for short in range(2):
                for way in range(2):
                    here = hops[short] - 1 - s
                    if here < 0:
                        continue
                    layer = layers[way][short]
                    mine = came[k].at[way, 2 * s + short]
                    with jax.named_scope(f"recv{s}{k}{short}{way}"):
                        sum_copy(way, short, s, k).wait_recv()
                    if k not in waited:
                        waited.add(k)
                        rest[k].wait()
                    term = block(held[k], layer, at(sign(way, here)), k)
                    if here > 0:

                        @pl.loop(0, rows[k] // TILE)
                        def _(t):
                            tile = pl.ds(pl.multiple_of(t * TILE, TILE), TILE)
                            mine[tile] = (mine[tile].astype(jnp.float32) + term[tile].astype(jnp.float32)).astype(jnp.bfloat16)

                        sum_copy(way, short, s, k).wait_send()
                        sum_copy(way, short, s + 1, k).start()
                    elif not short:
                        other, to = came[k].at[1 - way, 2 * (s - 1) + 1], total[k].at[layer]

                        def add(t, squares):
                            tile = pl.ds(pl.multiple_of(t * TILE, TILE), TILE)
                            g = term[tile].astype(jnp.float32) + mine[tile].astype(jnp.float32) + other[tile].astype(jnp.float32)
                            g = g.astype(jnp.bfloat16)
                            to[tile] = g
                            g = g.astype(jnp.float32)
                            g = g * g
                            for i in range(TILE // 8):
                                for c in range(g.shape[1] // 128):
                                    squares = squares + g[8 * i : 8 * i + 8, 128 * c : 128 * c + 128]
                            return squares

                        squares = lax.fori_loop(0, rows[k] // TILE, add, squares)

    def part_copy(away, sender):
        ref = parts.at[pl.ds(sender, 1)]
        return pltpu.make_async_remote_copy(
            src_ref=ref,
            dst_ref=ref,
            send_sem=part_sem.at[0],
            recv_sem=part_sem.at[1],
            device_id={"dp": at(away)},
            device_id_type=MESH,
        )

    with jax.named_scope("exchange"):
        parts[pl.ds(me, 1)] = jnp.sum(squares, axis=0, keepdims=True)
        for away in sorted(range(1, n), key=lambda away: -min(away, n - away)):
            part_copy(away, me).start()
        for copy in owns:
            copy.wait()
        for way in range(2):
            for short in range(2):
                for k in range(3):
                    sum_copy(way, short, hops[short] - 1, k).wait_send()
        others = parts.at[pl.ds(0, n - 1)]
        for i in range(2):
            pltpu.make_async_copy(others, others, part_sem.at[i]).wait()
    factor = jnp.minimum(1.0, 0.5 * lax.rsqrt(jnp.sum(parts[...], keepdims=True) / count + 1e-30))

    gather = Gather(n, towards, layers, hops, send_sem, recv_sem)
    last = len(weights) - 1
    for k in range(3):
        for layer in range(2):
            to = w_out[k].at[layer] if k == last else block(w_out[k], layer, me, k)

            with jax.named_scope(f"adamw{k}{layer}"):

                @pl.loop(0, rows[k] // TILE)
                def _(t):
                    tile = pl.ds(pl.multiple_of(t * TILE, TILE), TILE)
                    g = total[k][layer, tile].astype(jnp.float32) * factor
                    w, m, v = adamw(own[k][layer, tile].astype(jnp.float32), m_own[k][layer, tile], v_own[k][layer, tile], g)
                    to[tile] = w
                    m_out[k][layer, tile] = m
                    v_out[k][layer, tile] = v

            if k < last:
                for way in range(2):
                    gather.copy(w_out[k], way, int(layer != way), 0, k, me, rows[k]).start()
    gather.forward([(w_out[k], rows[k], 0, rows[k]) for k in range(last)])


def kernel_of_the_last(n, own, token, out, send_sem, recv_sem):
    del token
    me = lax.axis_index("dp")
    towards = (lax.rem(me + 1, n), lax.rem(me + n - 1, n))
    rows = own.shape[1]
    cut = rows // 2 // TILE * TILE
    cuts = [(0, rows - cut), (rows - cut, cut)]
    barrier = pltpu.get_barrier_semaphore()
    for peer in towards:
        pl.semaphore_signal(barrier, inc=1, device_id={"dp": peer}, device_id_type=MESH)
    first = pl.multiple_of(me * rows, rows)

    @pl.loop(0, rows // TILE)
    def _(t):
        tile = pl.multiple_of(t * TILE, TILE)
        for layer in range(2):
            out[layer, pl.ds(pl.multiple_of(first + tile, TILE), TILE)] = own[layer, pl.ds(tile, TILE)]

    pl.semaphore_wait(barrier, 2)
    gather = Gather(n, towards, [[way, 1 - way] for way in range(2)], [n // 2, n // 2 - 1], send_sem, recv_sem)
    for p, (start, size) in enumerate(cuts):
        for short in range(2):
            for way in range(2):
                source = own.at[gather.layers[way][short], pl.ds(start, size)]
                gather.copy(out, way, short, 0, p, me, rows, start, size, source).start()
    gather.forward([(out, rows, *cut) for cut in cuts], own)


def flush(count, *refs):
    sem, tokens = refs[-1], refs[2 * count : -1]
    copies = [pltpu.make_async_copy(refs[i], refs[count + i], sem.at[i]) for i in range(count)]
    for copy in copies:
        copy.start()
    for token in tokens:
        token[...] = jnp.zeros_like(token)
    for copy in copies:
        copy.wait()


def flushed(arrays, *tokens):
    count = len(arrays)
    return pl.pallas_call(
        functools.partial(flush, count),
        name="flush",
        out_shape=[*(jax.ShapeDtypeStruct(a.shape, a.dtype) for a in arrays), *tokens],
        in_specs=[pl.BlockSpec(memory_space=pltpu.VMEM)] * count,
        out_specs=[pl.BlockSpec(memory_space=pl.ANY)] * count + [pl.BlockSpec(memory_space=pltpu.VMEM)] * len(tokens),
        scratch_shapes=[pltpu.SemaphoreType.DMA((count,))],
        compiler_params=pltpu.CompilerParams(vmem_limit_bytes=2**20),
    )(*arrays)


def solution(mesh):
    def step(*arrays):
        n = lax.axis_size("dp")
        terms, weights, m, v = (arrays[i : i + 3] for i in (0, 3, 6, 9))
        count = sum(w.size for w in weights)
        shapes = [(w.shape, w.dtype) for w in weights[:-1]] + [(m[-1].shape, weights[-1].dtype)] + [(x.shape, x.dtype) for x in (*m, *v)]
        blocks = [(one.shape[1], one.shape[2]) for one in m]
        half = n // 2
        outs = pl.pallas_call(
            functools.partial(kernel, n, count),
            name="step",
            out_shape=[pltpu.VMEM(s, d) for s, d in shapes],
            in_specs=[pl.BlockSpec(memory_space=pl.ANY)] * 12,
            out_specs=[pl.BlockSpec(memory_space=pltpu.VMEM)] * 9,
            scratch_shapes=[
                *(pltpu.VMEM((2, 2, *b), jnp.bfloat16) for b in blocks),
                *(pltpu.VMEM(w.shape, jnp.bfloat16) for w in weights),
                *(pltpu.VMEM((2, 2 * half - 1, *b), jnp.bfloat16) for b in blocks),
                *(pltpu.VMEM((2, *b), jnp.bfloat16) for b in blocks),
                *(pltpu.VMEM((2, *b), jnp.float32) for b in blocks * 2),
                *(pltpu.VMEM((2, *b), jnp.bfloat16) for b in blocks),
                pltpu.VMEM((n, 128), jnp.float32),
                pltpu.SemaphoreType.DMA((4,)),
                pltpu.SemaphoreType.DMA((3, 3)),
                pltpu.SemaphoreType.DMA((2, 2, 3)),
                pltpu.SemaphoreType.DMA((2, 2 * half - 1, 3)),
                pltpu.SemaphoreType.DMA((2,)),
            ],
            compiler_params=pltpu.CompilerParams(collective_id=0, has_side_effects=True, vmem_limit_bytes=48 * 2**20),
        )(*arrays)
        *whole, own, m0, m1, m2, v0, v1, v2 = outs
        *done, token = flushed([*whole, m0, m1, m2, v0, v1, v2], pltpu.VMEM((8, 128), jnp.float32))
        last = pl.pallas_call(
            functools.partial(kernel_of_the_last, n),
            name="last",
            out_shape=pltpu.VMEM(weights[-1].shape, weights[-1].dtype),
            in_specs=[pl.BlockSpec(memory_space=pltpu.VMEM)] * 2,
            out_specs=pl.BlockSpec(memory_space=pltpu.VMEM),
            scratch_shapes=[pltpu.SemaphoreType.DMA((2, 2, 2)), pltpu.SemaphoreType.DMA((2, 2 * half - 1, 2))],
            compiler_params=pltpu.CompilerParams(collective_id=1, has_side_effects=True, vmem_limit_bytes=2**20),
        )(own, token)
        return (*done[: len(whole)], *flushed([last]), *done[len(whole) :])

    all_of, cut = P(None, None, None), P(None, "dp", None)
    return jax.shard_map(
        step,
        mesh=mesh,
        in_specs=(P(("rep", "dp"), None, None, None),) * 3 + (all_of,) * 3 + (cut,) * 6,
        out_specs=(P("rep", None, None),) * 3 + (P("rep", "dp", None),) * 6,
        check_vma=False,
    )
```

```python
import functools

import jax
import jax.numpy as jnp
from jax import lax
from jax.experimental import pallas as pl
from jax.experimental.pallas import tpu as pltpu
from jax.sharding import PartitionSpec as P

MESH = pl.DeviceIdType.MESH
TILE = 16
PIECES = 2
LATER = 9500


def adamw(w, m, v, g):
    m = 0.9 * m + 0.1 * g
    v = 0.95 * v + 0.05 * g * g
    step = m * lax.rsqrt(v + 1e-8) + 0.1 * w
    return (w - 0.02 * step).astype(jnp.bfloat16), m, v


def all_of_it(ref, sem):
    pltpu.make_async_copy(ref, ref, sem).wait()


class Gather:
    def __init__(self, n, towards, layers, hops, send_sem, recv_sem):
        self.n, self.towards, self.layers, self.hops = n, towards, layers, hops
        self.send_sem, self.recv_sem = send_sem, recv_sem
        self.me = lax.axis_index("dp")

    def behind(self, way, s):
        return lax.rem(self.me + (-s if way == 0 else s) + self.n, self.n)

    def copy(self, ref, way, short, s, p, sender, rows, start=0, size=None, source=None):
        to = ref.at[self.layers[way][short], pl.ds(pl.multiple_of(sender * rows + start, TILE), size or rows)]
        return pltpu.make_async_remote_copy(
            src_ref=to if source is None else source,
            dst_ref=to,
            send_sem=self.send_sem.at[way, p],
            recv_sem=self.recv_sem.at[way, 2 * s + short, p],
            device_id={"dp": self.towards[way]},
            device_id_type=MESH,
        )

    def forward(self, pieces, order):
        for s in range(self.hops[0]):
            for p, short in order:
                ref, rows, start, size = pieces[p]
                for way in range(2):
                    if s >= self.hops[short]:
                        continue

                    def copy(step, behind):
                        return self.copy(ref, way, short, step, p, self.behind(way, behind), rows, start, size)

                    with jax.named_scope(f"get{s}{p}{short}{way}"):
                        copy(s, s + 1).wait_recv()
                    if s + 1 < self.hops[short]:
                        copy(s + 1, s + 1).start()


def kernel(n, count, *refs):
    terms, weights, m_in, v_in = (refs[i : i + 3] for i in (0, 3, 6, 9))
    w_out, m_out, v_out = (refs[i : i + 3] for i in (12, 15, 18))
    raw, held, came, own, m_own, v_own, total = (refs[i : i + 3] for i in range(21, 42, 3))
    parts, load_sem, own_sem, send_sem, recv_sem, part_sem = refs[42:]
    me = lax.axis_index("dp")
    rows = [m.shape[1] for m in m_in]
    half = n // 2

    def at(away):
        return lax.rem(me + away + n, n)

    def sign(way, away):
        return away if way == 0 else -away

    def block(ref, layer, who, k):
        return ref.at[layer, pl.ds(pl.multiple_of(who * rows[k], rows[k]), rows[k])]

    towards = (at(1), at(-1))
    layers = [[way, 1 - way] for way in range(2)]
    hops = [half, half - 1]

    barrier = pltpu.get_barrier_semaphore()
    for peer in towards:
        pl.semaphore_signal(barrier, inc=1, device_id={"dp": peer}, device_id_type=MESH)

    def first(way, short, k, sem):
        source = block(terms[k].at[0], layers[way][short], at(sign(way, hops[short])), k)
        return pltpu.make_async_copy(source, raw[k].at[way, short], load_sem.at[sem])

    rest = [pltpu.make_async_copy(terms[k].at[0], held[k], load_sem.at[k]) for k in range(3)]
    owns = [
        pltpu.make_async_copy(source, to, own_sem.at[i, k])
        for k in range(3)
        for i, (source, to) in enumerate(
            [(weights[k].at[:, pl.ds(pl.multiple_of(me * rows[k], rows[k]), rows[k])], own[k]), (m_in[k], m_own[k]), (v_in[k], v_own[k])]
        )
    ]
    pl.semaphore_wait(barrier, 2)
    for k in range(3):
        for short in range(k == 0, 2):
            for way in range(2):
                first(way, short, k, k).start()

    @pl.when(lax.rem(lax.axis_index("rep"), 2) == 0)
    def _():
        pl.delay(LATER)

    def send(way, short, s, k, source, to):
        return pltpu.make_async_remote_copy(
            src_ref=source,
            dst_ref=to,
            send_sem=send_sem.at[way, k],
            recv_sem=recv_sem.at[way, 2 * s + short, k],
            device_id={"dp": towards[way]},
            device_id_type=MESH,
        )

    def sum_copy(way, short, s, k):
        source = raw[k].at[way, short] if s == 0 else came[k].at[way, 2 * (s - 1) + short]
        if s == k == short == 0:
            source = block(terms[k].at[0], layers[way][short], at(sign(way, hops[short])), k)
        return send(way, short, s, k, source, came[k].at[way, 2 * s + short])

    with jax.named_scope("first"):
        for k in range(3):
            for short in range(2):
                if short if k == 0 else not short:
                    ready = raw[k] if k else raw[k].at[:, short]
                    all_of_it(ready, load_sem.at[0 if short else (3, 1, 2)[k]])
                for way in range(2):
                    sum_copy(way, short, 0, k).start()
            rest[k].start()
        for copy in owns:
            copy.start()

    squares = jnp.zeros((8, 128), jnp.float32)
    waited = set()
    for s in range(half):
        for k in range(3):
            for short in range(2):
                for way in range(2):
                    here = hops[short] - 1 - s
                    if here < 0:
                        continue
                    layer = layers[way][short]
                    mine = came[k].at[way, 2 * s + short]
                    with jax.named_scope(f"recv{s}{k}{short}{way}"):
                        sum_copy(way, short, s, k).wait_recv()
                    if k not in waited:
                        waited.add(k)
                        rest[k].wait()
                    term = block(held[k], layer, at(sign(way, here)), k)
                    if here > 0:

                        @pl.loop(0, rows[k] // TILE)
                        def _(t):
                            tile = pl.ds(pl.multiple_of(t * TILE, TILE), TILE)
                            mine[tile] = (mine[tile].astype(jnp.float32) + term[tile].astype(jnp.float32)).astype(jnp.bfloat16)

                        sum_copy(way, short, s + 1, k).start()
                    elif not short:
                        other, to = came[k].at[1 - way, 2 * (s - 1) + 1], total[k].at[layer]

                        def add(t, squares):
                            tile = pl.ds(pl.multiple_of(t * TILE, TILE), TILE)
                            g = term[tile].astype(jnp.float32) + mine[tile].astype(jnp.float32) + other[tile].astype(jnp.float32)
                            g = g.astype(jnp.bfloat16)
                            to[tile] = g
                            g = g.astype(jnp.float32)
                            g = g * g
                            for i in range(TILE // 8):
                                for c in range(g.shape[1] // 128):
                                    squares = squares + g[8 * i : 8 * i + 8, 128 * c : 128 * c + 128]
                            return squares

                        squares = lax.fori_loop(0, rows[k] // TILE, add, squares)

    def part_copy(away, sender):
        ref = parts.at[pl.ds(sender, 1)]
        return pltpu.make_async_remote_copy(
            src_ref=ref,
            dst_ref=ref,
            send_sem=part_sem.at[0],
            recv_sem=part_sem.at[1],
            device_id={"dp": at(away)},
            device_id_type=MESH,
        )

    with jax.named_scope("exchange"):
        parts[pl.ds(me, 1)] = jnp.sum(squares, axis=0, keepdims=True)
        for away in sorted(range(1, n), key=lambda away: -min(away, n - away)):
            part_copy(away, me).start()
        for copy in owns:
            copy.wait()
        for way in range(2):
            for k in range(3):
                all_of_it(came[k].at[way], send_sem.at[way, k])
        others = parts.at[pl.ds(0, n - 1)]
        for i in range(2):
            all_of_it(others, part_sem.at[i])
    factor = jnp.minimum(1.0, 0.5 * lax.rsqrt(jnp.sum(parts[...], keepdims=True) / count + 1e-30))

    gather = Gather(n, towards, layers, hops, send_sem, recv_sem)
    last = len(weights) - 1
    for k in range(3):
        for layer in range(2):
            to = w_out[k].at[layer] if k == last else block(w_out[k], layer, me, k)

            with jax.named_scope(f"adamw{k}{layer}"):

                @pl.loop(0, rows[k] // TILE)
                def _(t):
                    tile = pl.ds(pl.multiple_of(t * TILE, TILE), TILE)
                    g = total[k][layer, tile].astype(jnp.float32) * factor
                    w, m, v = adamw(own[k][layer, tile].astype(jnp.float32), m_own[k][layer, tile], v_own[k][layer, tile], g)
                    to[tile] = w
                    m_out[k][layer, tile] = m
                    v_out[k][layer, tile] = v

            if k < last:
                for way in range(2):
                    gather.copy(w_out[k], way, int(layer != way), 0, k, me, rows[k]).start()
    gather.forward([(w_out[k], rows[k], 0, rows[k]) for k in range(last)], [(k, short) for k in range(last) for short in range(2)])
    for way in range(2):
        for k in range(last):
            all_of_it(came[k].at[way], send_sem.at[way, k])


def kernel_of_the_last(n, own, token, out, send_sem, recv_sem):
    del token
    me = lax.axis_index("dp")
    towards = (lax.rem(me + 1, n), lax.rem(me + n - 1, n))
    rows = own.shape[1]
    edges = [rows // TILE * p // PIECES * TILE for p in range(PIECES + 1)]
    cuts = [(start, end - start) for start, end in zip(edges, edges[1:])]
    order = [(p, short) for short in range(2) for p in range(PIECES)]
    barrier = pltpu.get_barrier_semaphore()
    for peer in towards:
        pl.semaphore_signal(barrier, inc=1, device_id={"dp": peer}, device_id_type=MESH)
    first = pl.multiple_of(me * rows, rows)

    @pl.loop(0, rows // TILE)
    def _(t):
        tile = pl.multiple_of(t * TILE, TILE)
        for layer in range(2):
            out[layer, pl.ds(pl.multiple_of(first + tile, TILE), TILE)] = own[layer, pl.ds(tile, TILE)]

    pl.semaphore_wait(barrier, 2)
    gather = Gather(n, towards, [[way, 1 - way] for way in range(2)], [n // 2, n // 2 - 1], send_sem, recv_sem)
    for p, short in order:
        start, size = cuts[p]
        for way in range(2):
            source = own.at[gather.layers[way][short], pl.ds(start, size)]
            gather.copy(out, way, short, 0, p, me, rows, start, size, source).start()
    gather.forward([(out, rows, *cut) for cut in cuts], order)
    for way in range(2):
        for p, (_, size) in enumerate(cuts):
            all_of_it(out.at[0, pl.ds(0, sum(gather.hops) * size)], send_sem.at[way, p])


def flush(count, *refs):
    sem, tokens = refs[-1], refs[2 * count : -1]
    copies = [pltpu.make_async_copy(refs[i], refs[count + i], sem.at[i]) for i in range(count)]
    for copy in copies:
        copy.start()
    for token in tokens:
        token[...] = jnp.zeros_like(token)
    for copy in copies:
        copy.wait()


def flushed(arrays, *tokens):
    count = len(arrays)
    return pl.pallas_call(
        functools.partial(flush, count),
        name="flush",
        out_shape=[*(jax.ShapeDtypeStruct(a.shape, a.dtype) for a in arrays), *tokens],
        in_specs=[pl.BlockSpec(memory_space=pltpu.VMEM)] * count,
        out_specs=[pl.BlockSpec(memory_space=pl.ANY)] * count + [pl.BlockSpec(memory_space=pltpu.VMEM)] * len(tokens),
        scratch_shapes=[pltpu.SemaphoreType.DMA((count,))],
        compiler_params=pltpu.CompilerParams(vmem_limit_bytes=2**20),
    )(*arrays)


def solution(mesh):
    def step(*arrays):
        n = lax.axis_size("dp")
        terms, weights, m, v = (arrays[i : i + 3] for i in (0, 3, 6, 9))
        count = sum(w.size for w in weights)
        shapes = [(w.shape, w.dtype) for w in weights[:-1]] + [(m[-1].shape, weights[-1].dtype)] + [(x.shape, x.dtype) for x in (*m, *v)]
        blocks = [(one.shape[1], one.shape[2]) for one in m]
        half = n // 2
        outs = pl.pallas_call(
            functools.partial(kernel, n, count),
            name="step",
            out_shape=[pltpu.VMEM(s, d) for s, d in shapes],
            in_specs=[pl.BlockSpec(memory_space=pl.ANY)] * 12,
            out_specs=[pl.BlockSpec(memory_space=pltpu.VMEM)] * 9,
            scratch_shapes=[
                *(pltpu.VMEM((2, 2, *b), jnp.bfloat16) for b in blocks),
                *(pltpu.VMEM(w.shape, jnp.bfloat16) for w in weights),
                *(pltpu.VMEM((2, 2 * half - 1, *b), jnp.bfloat16) for b in blocks),
                *(pltpu.VMEM((2, *b), jnp.bfloat16) for b in blocks),
                *(pltpu.VMEM((2, *b), jnp.float32) for b in blocks * 2),
                *(pltpu.VMEM((2, *b), jnp.bfloat16) for b in blocks),
                pltpu.VMEM((n, 128), jnp.float32),
                pltpu.SemaphoreType.DMA((4,)),
                pltpu.SemaphoreType.DMA((3, 3)),
                pltpu.SemaphoreType.DMA((2, 3)),
                pltpu.SemaphoreType.DMA((2, 2 * half - 1, 3)),
                pltpu.SemaphoreType.DMA((2,)),
            ],
            compiler_params=pltpu.CompilerParams(collective_id=0, has_side_effects=True, vmem_limit_bytes=48 * 2**20),
        )(*arrays)
        *whole, own, m0, m1, m2, v0, v1, v2 = outs
        *done, token = flushed([*whole, m0, m1, m2, v0, v1, v2], pltpu.VMEM((8, 128), jnp.float32))
        last = pl.pallas_call(
            functools.partial(kernel_of_the_last, n),
            name="last",
            out_shape=pltpu.VMEM(weights[-1].shape, weights[-1].dtype),
            in_specs=[pl.BlockSpec(memory_space=pltpu.VMEM)] * 2,
            out_specs=pl.BlockSpec(memory_space=pltpu.VMEM),
            scratch_shapes=[pltpu.SemaphoreType.DMA((2, PIECES)), pltpu.SemaphoreType.DMA((2, 2 * half - 1, PIECES))],
            compiler_params=pltpu.CompilerParams(collective_id=1, has_side_effects=True, vmem_limit_bytes=2**20),
        )(own, token)
        return (*done[: len(whole)], *flushed([last]), *done[len(whole) :])

    all_of, cut = P(None, None, None), P(None, "dp", None)
    return jax.shard_map(
        step,
        mesh=mesh,
        in_specs=(P(("rep", "dp"), None, None, None),) * 3 + (all_of,) * 3 + (cut,) * 6,
        out_specs=(P("rep", None, None),) * 3 + (P("rep", "dp", None),) * 6,
        check_vma=False,
    )
```

```python
import functools

import jax
import jax.numpy as jnp
from jax import lax
from jax.experimental import pallas as pl
from jax.experimental.pallas import tpu as pltpu
from jax.sharding import PartitionSpec as P

MESH = pl.DeviceIdType.MESH
TILE = 16
PIECES = 2
LATER = 9500


def adamw(w, m, v, g):
    m = 0.9 * m + 0.1 * g
    v = 0.95 * v + 0.05 * g * g
    step = m * lax.rsqrt(v + 1e-8) + 0.1 * w
    return (w - 0.02 * step).astype(jnp.bfloat16), m, v


def all_of_it(ref, sem):
    pltpu.make_async_copy(ref, ref, sem).wait()


class Gather:
    def __init__(self, n, towards, layers, hops, send_sem, recv_sem):
        self.n, self.towards, self.layers, self.hops = n, towards, layers, hops
        self.send_sem, self.recv_sem = send_sem, recv_sem
        self.me = lax.axis_index("dp")

    def behind(self, way, s):
        return lax.rem(self.me + (-s if way == 0 else s) + self.n, self.n)

    def copy(self, ref, way, short, s, p, sender, rows, start=0, size=None, source=None):
        to = ref.at[self.layers[way][short], pl.ds(pl.multiple_of(sender * rows + start, TILE), size or rows)]
        return pltpu.make_async_remote_copy(
            src_ref=to if source is None else source,
            dst_ref=to,
            send_sem=self.send_sem.at[way, p],
            recv_sem=self.recv_sem.at[way, 2 * s + short, p],
            device_id={"dp": self.towards[way]},
            device_id_type=MESH,
        )

    def forward(self, pieces, order):
        for s in range(self.hops[0]):
            for p, short in order:
                ref, rows, start, size = pieces[p]
                for way in range(2):
                    if s >= self.hops[short]:
                        continue

                    def copy(step, behind):
                        return self.copy(ref, way, short, step, p, self.behind(way, behind), rows, start, size)

                    copy(s, s + 1).wait_recv()
                    if s + 1 < self.hops[short]:
                        copy(s + 1, s + 1).start()


def kernel(n, count, *refs):
    terms, weights, m_in, v_in = (refs[i : i + 3] for i in (0, 3, 6, 9))
    w_out, m_out, v_out = (refs[i : i + 3] for i in (12, 15, 18))
    raw, held, came, own, m_own, v_own, total = (refs[i : i + 3] for i in range(21, 42, 3))
    parts, load_sem, own_sem, send_sem, recv_sem, part_sem = refs[42:]
    me = lax.axis_index("dp")
    rows = [m.shape[1] for m in m_in]
    half = n // 2

    def at(away):
        return lax.rem(me + away + n, n)

    def sign(way, away):
        return away if way == 0 else -away

    def block(ref, layer, who, k):
        return ref.at[layer, pl.ds(pl.multiple_of(who * rows[k], rows[k]), rows[k])]

    towards = (at(1), at(-1))
    layers = [[way, 1 - way] for way in range(2)]
    hops = [half, half - 1]

    barrier = pltpu.get_barrier_semaphore()
    for peer in towards:
        pl.semaphore_signal(barrier, inc=1, device_id={"dp": peer}, device_id_type=MESH)

    def begins(way, short, k):
        return block(terms[k].at[0], layers[way][short], at(sign(way, hops[short])), k)

    rest = [pltpu.make_async_copy(terms[k].at[0], held[k], load_sem.at[k]) for k in range(3)]
    owns = [
        pltpu.make_async_copy(source, to, own_sem.at[i, k])
        for k in range(3)
        for i, (source, to) in enumerate(
            [(weights[k].at[:, pl.ds(pl.multiple_of(me * rows[k], rows[k]), rows[k])], own[k]), (m_in[k], m_own[k]), (v_in[k], v_own[k])]
        )
    ]
    pl.semaphore_wait(barrier, 2)
    for k in range(3):
        for short in range(k == 0, 2):
            for way in range(2):
                pltpu.make_async_copy(begins(way, short, k), raw[k].at[way, short], load_sem.at[k]).start()

    @pl.when(lax.rem(lax.axis_index("rep"), 2) == 0)
    def _():
        pl.delay(LATER)

    def send(way, short, s, k, source, to):
        return pltpu.make_async_remote_copy(
            src_ref=source,
            dst_ref=to,
            send_sem=send_sem.at[way, k],
            recv_sem=recv_sem.at[way, 2 * s + short, k],
            device_id={"dp": towards[way]},
            device_id_type=MESH,
        )

    def sum_copy(way, short, s, k):
        if s:
            source = came[k].at[way, 2 * (s - 1) + short]
        else:
            source = raw[k].at[way, short] if k or short else begins(way, short, k)
        return send(way, short, s, k, source, came[k].at[way, 2 * s + short])

    for way in range(2):
        sum_copy(way, 0, 0, 0).start()
    for k in range(3):
        all_of_it(raw[k] if k else raw[k].at[:, 1], load_sem.at[k])
        for short in range(k == 0, 2):
            for way in range(2):
                sum_copy(way, short, 0, k).start()
        rest[k].start()
    for copy in owns:
        copy.start()

    squares = jnp.zeros((8, 128), jnp.float32)
    waited = set()
    for s in range(half):
        for k in range(3):
            for short in range(2):
                for way in range(2):
                    here = hops[short] - 1 - s
                    if here < 0:
                        continue
                    layer = layers[way][short]
                    mine = came[k].at[way, 2 * s + short]
                    sum_copy(way, short, s, k).wait_recv()
                    if k not in waited:
                        waited.add(k)
                        rest[k].wait()
                    term = block(held[k], layer, at(sign(way, here)), k)
                    if here > 0:

                        @pl.loop(0, rows[k] // TILE)
                        def _(t):
                            tile = pl.ds(pl.multiple_of(t * TILE, TILE), TILE)
                            mine[tile] = (mine[tile].astype(jnp.float32) + term[tile].astype(jnp.float32)).astype(jnp.bfloat16)

                        sum_copy(way, short, s + 1, k).start()
                    elif not short:
                        other, to = came[k].at[1 - way, 2 * (s - 1) + 1], total[k].at[layer]

                        def add(t, squares):
                            tile = pl.ds(pl.multiple_of(t * TILE, TILE), TILE)
                            g = term[tile].astype(jnp.float32) + mine[tile].astype(jnp.float32) + other[tile].astype(jnp.float32)
                            g = g.astype(jnp.bfloat16)
                            to[tile] = g
                            g = g.astype(jnp.float32)
                            g = g * g
                            for i in range(TILE // 8):
                                for c in range(g.shape[1] // 128):
                                    squares = squares + g[8 * i : 8 * i + 8, 128 * c : 128 * c + 128]
                            return squares

                        squares = lax.fori_loop(0, rows[k] // TILE, add, squares)

    def part_copy(away, sender):
        ref = parts.at[pl.ds(sender, 1)]
        return pltpu.make_async_remote_copy(
            src_ref=ref,
            dst_ref=ref,
            send_sem=part_sem.at[0],
            recv_sem=part_sem.at[1],
            device_id={"dp": at(away)},
            device_id_type=MESH,
        )

    parts[pl.ds(me, 1)] = jnp.sum(squares, axis=0, keepdims=True)
    for away in sorted(range(1, n), key=lambda away: -min(away, n - away)):
        part_copy(away, me).start()
    for copy in owns:
        copy.wait()
    for way in range(2):
        for k in range(3):
            all_of_it(came[k].at[way], send_sem.at[way, k])
    others = parts.at[pl.ds(0, n - 1)]
    for i in range(2):
        all_of_it(others, part_sem.at[i])
    factor = jnp.minimum(1.0, 0.5 * lax.rsqrt(jnp.sum(parts[...], keepdims=True) / count + 1e-30))

    gather = Gather(n, towards, layers, hops, send_sem, recv_sem)
    last = len(weights) - 1
    for k in range(3):
        for layer in range(2):
            to = w_out[k].at[layer] if k == last else block(w_out[k], layer, me, k)


            @pl.loop(0, rows[k] // TILE)
            def _(t):
                tile = pl.ds(pl.multiple_of(t * TILE, TILE), TILE)
                g = total[k][layer, tile].astype(jnp.float32) * factor
                w, m, v = adamw(own[k][layer, tile].astype(jnp.float32), m_own[k][layer, tile], v_own[k][layer, tile], g)
                to[tile] = w
                m_out[k][layer, tile] = m
                v_out[k][layer, tile] = v

            if k < last:
                for way in range(2):
                    gather.copy(w_out[k], way, int(layer != way), 0, k, me, rows[k]).start()
    gather.forward([(w_out[k], rows[k], 0, rows[k]) for k in range(last)], [(k, short) for k in range(last) for short in range(2)])
    for way in range(2):
        for k in range(last):
            all_of_it(came[k].at[way], send_sem.at[way, k])


def kernel_of_the_last(n, own, token, out, send_sem, recv_sem):
    del token
    me = lax.axis_index("dp")
    towards = (lax.rem(me + 1, n), lax.rem(me + n - 1, n))
    rows = own.shape[1]
    edges = [rows // TILE * p // PIECES * TILE for p in range(PIECES + 1)]
    cuts = [(start, end - start) for start, end in zip(edges, edges[1:])]
    order = [(p, short) for short in range(2) for p in range(PIECES)]
    barrier = pltpu.get_barrier_semaphore()
    for peer in towards:
        pl.semaphore_signal(barrier, inc=1, device_id={"dp": peer}, device_id_type=MESH)
    first = pl.multiple_of(me * rows, rows)

    @pl.loop(0, rows // TILE)
    def _(t):
        tile = pl.multiple_of(t * TILE, TILE)
        for layer in range(2):
            out[layer, pl.ds(pl.multiple_of(first + tile, TILE), TILE)] = own[layer, pl.ds(tile, TILE)]

    pl.semaphore_wait(barrier, 2)
    gather = Gather(n, towards, [[way, 1 - way] for way in range(2)], [n // 2, n // 2 - 1], send_sem, recv_sem)
    for p, short in order:
        start, size = cuts[p]
        for way in range(2):
            source = own.at[gather.layers[way][short], pl.ds(start, size)]
            gather.copy(out, way, short, 0, p, me, rows, start, size, source).start()
    gather.forward([(out, rows, *cut) for cut in cuts], order)
    for way in range(2):
        for p, (_, size) in enumerate(cuts):
            all_of_it(out.at[0, pl.ds(0, sum(gather.hops) * size)], send_sem.at[way, p])


def flush(count, *refs):
    sem, tokens = refs[-1], refs[2 * count : -1]
    copies = [pltpu.make_async_copy(refs[i], refs[count + i], sem.at[i]) for i in range(count)]
    for copy in copies:
        copy.start()
    for token in tokens:
        token[...] = jnp.zeros_like(token)
    for copy in copies:
        copy.wait()


def flushed(arrays, *tokens):
    count = len(arrays)
    return pl.pallas_call(
        functools.partial(flush, count),
        name="flush",
        out_shape=[*(jax.ShapeDtypeStruct(a.shape, a.dtype) for a in arrays), *tokens],
        in_specs=[pl.BlockSpec(memory_space=pltpu.VMEM)] * count,
        out_specs=[pl.BlockSpec(memory_space=pl.ANY)] * count + [pl.BlockSpec(memory_space=pltpu.VMEM)] * len(tokens),
        scratch_shapes=[pltpu.SemaphoreType.DMA((count,))],
        compiler_params=pltpu.CompilerParams(vmem_limit_bytes=2**20),
    )(*arrays)


def solution(mesh):
    def step(*arrays):
        n = lax.axis_size("dp")
        terms, weights, m, v = (arrays[i : i + 3] for i in (0, 3, 6, 9))
        count = sum(w.size for w in weights)
        shapes = [(w.shape, w.dtype) for w in weights[:-1]] + [(m[-1].shape, weights[-1].dtype)] + [(x.shape, x.dtype) for x in (*m, *v)]
        blocks = [(one.shape[1], one.shape[2]) for one in m]
        half = n // 2
        outs = pl.pallas_call(
            functools.partial(kernel, n, count),
            name="step",
            out_shape=[pltpu.VMEM(s, d) for s, d in shapes],
            in_specs=[pl.BlockSpec(memory_space=pl.ANY)] * 12,
            out_specs=[pl.BlockSpec(memory_space=pltpu.VMEM)] * 9,
            scratch_shapes=[
                *(pltpu.VMEM((2, 2, *b), jnp.bfloat16) for b in blocks),
                *(pltpu.VMEM(w.shape, jnp.bfloat16) for w in weights),
                *(pltpu.VMEM((2, 2 * half - 1, *b), jnp.bfloat16) for b in blocks),
                *(pltpu.VMEM((2, *b), jnp.bfloat16) for b in blocks),
                *(pltpu.VMEM((2, *b), jnp.float32) for b in blocks * 2),
                *(pltpu.VMEM((2, *b), jnp.bfloat16) for b in blocks),
                pltpu.VMEM((n, 128), jnp.float32),
                pltpu.SemaphoreType.DMA((3,)),
                pltpu.SemaphoreType.DMA((3, 3)),
                pltpu.SemaphoreType.DMA((2, 3)),
                pltpu.SemaphoreType.DMA((2, 2 * half - 1, 3)),
                pltpu.SemaphoreType.DMA((2,)),
            ],
            compiler_params=pltpu.CompilerParams(collective_id=0, has_side_effects=True, vmem_limit_bytes=48 * 2**20),
        )(*arrays)
        *whole, own, m0, m1, m2, v0, v1, v2 = outs
        *done, token = flushed([*whole, m0, m1, m2, v0, v1, v2], pltpu.VMEM((8, 128), jnp.float32))
        last = pl.pallas_call(
            functools.partial(kernel_of_the_last, n),
            name="last",
            out_shape=pltpu.VMEM(weights[-1].shape, weights[-1].dtype),
            in_specs=[pl.BlockSpec(memory_space=pltpu.VMEM)] * 2,
            out_specs=pl.BlockSpec(memory_space=pltpu.VMEM),
            scratch_shapes=[pltpu.SemaphoreType.DMA((2, PIECES)), pltpu.SemaphoreType.DMA((2, 2 * half - 1, PIECES))],
            compiler_params=pltpu.CompilerParams(collective_id=1, has_side_effects=True, vmem_limit_bytes=2**20),
        )(own, token)
        return (*done[: len(whole)], *flushed([last]), *done[len(whole) :])

    all_of, cut = P(None, None, None), P(None, "dp", None)
    return jax.shard_map(
        step,
        mesh=mesh,
        in_specs=(P(("rep", "dp"), None, None, None),) * 3 + (all_of,) * 3 + (cut,) * 6,
        out_specs=(P("rep", None, None),) * 3 + (P("rep", "dp", None),) * 6,
        check_vma=False,
    )
```

```python
import functools

import jax
import jax.numpy as jnp
from jax import lax
from jax.experimental import pallas as pl
from jax.experimental.pallas import tpu as pltpu
from jax.sharding import PartitionSpec as P

MESH = pl.DeviceIdType.MESH
TILE = 16
PIECES = 2
LATER = 9500


def adamw(w, m, v, g):
    m = 0.9 * m + 0.1 * g
    v = 0.95 * v + 0.05 * g * g
    step = m * lax.rsqrt(v + 1e-8) + 0.1 * w
    return (w - 0.02 * step).astype(jnp.bfloat16), m, v


def all_of_it(ref, sem):
    pltpu.make_async_copy(ref, ref, sem).wait()


class Gather:
    def __init__(self, n, towards, layers, hops, send_sem, recv_sem):
        self.n, self.towards, self.layers, self.hops = n, towards, layers, hops
        self.send_sem, self.recv_sem = send_sem, recv_sem
        self.me = lax.axis_index("dp")

    def behind(self, way, s):
        return lax.rem(self.me + (-s if way == 0 else s) + self.n, self.n)

    def copy(self, ref, way, short, s, p, sender, rows, start=0, size=None, source=None):
        to = ref.at[self.layers[way][short], pl.ds(pl.multiple_of(sender * rows + start, TILE), size or rows)]
        return pltpu.make_async_remote_copy(
            src_ref=to if source is None else source,
            dst_ref=to,
            send_sem=self.send_sem.at[way, p],
            recv_sem=self.recv_sem.at[way, 2 * s + short, p],
            device_id={"dp": self.towards[way]},
            device_id_type=MESH,
        )

    def forward(self, pieces, order):
        for s in range(self.hops[0]):
            for p, short in order:
                ref, rows, start, size = pieces[p]
                for way in range(2):
                    if s >= self.hops[short]:
                        continue

                    def copy(step, behind):
                        return self.copy(ref, way, short, step, p, self.behind(way, behind), rows, start, size)

                    copy(s, s + 1).wait_recv()
                    if s + 1 < self.hops[short]:
                        copy(s + 1, s + 1).start()


def kernel(n, count, *refs):
    terms, weights, m_in, v_in = (refs[i : i + 3] for i in (0, 3, 6, 9))
    w_out, m_out, v_out = (refs[i : i + 3] for i in (12, 15, 18))
    raw, held, came, own, m_own, v_own, total = (refs[i : i + 3] for i in range(21, 42, 3))
    parts, load_sem, own_sem, send_sem, recv_sem, part_sem = refs[42:]
    me = lax.axis_index("dp")
    rows = [m.shape[1] for m in m_in]
    half = n // 2

    def at(away):
        return lax.rem(me + away + n, n)

    def sign(way, away):
        return away if way == 0 else -away

    def block(ref, layer, who, k):
        return ref.at[layer, pl.ds(pl.multiple_of(who * rows[k], rows[k]), rows[k])]

    towards = (at(1), at(-1))
    layers = [[way, 1 - way] for way in range(2)]
    hops = [half, half - 1]

    barrier = pltpu.get_barrier_semaphore()
    for peer in towards:
        pl.semaphore_signal(barrier, inc=1, device_id={"dp": peer}, device_id_type=MESH)

    def begins(way, short, k):
        return block(terms[k].at[0], layers[way][short], at(sign(way, hops[short])), k)

    rest = [pltpu.make_async_copy(terms[k].at[0], held[k], load_sem.at[k]) for k in range(3)]
    owns = [
        pltpu.make_async_copy(source, to, own_sem.at[i, k])
        for k in range(3)
        for i, (source, to) in enumerate(
            [(weights[k].at[:, pl.ds(pl.multiple_of(me * rows[k], rows[k]), rows[k])], own[k]), (m_in[k], m_own[k]), (v_in[k], v_own[k])]
        )
    ]
    pl.semaphore_wait(barrier, 2)
    for k in range(3):
        for short in range(k == 0, 2):
            for way in range(2):
                pltpu.make_async_copy(begins(way, short, k), raw[k].at[way, short], load_sem.at[k]).start()

    @pl.when(lax.rem(lax.axis_index("rep"), 2) == 0)
    def _():
        pl.delay(LATER)

    def send(way, short, s, k, source, to):
        return pltpu.make_async_remote_copy(
            src_ref=source,
            dst_ref=to,
            send_sem=send_sem.at[way, k],
            recv_sem=recv_sem.at[way, 2 * s + short, k],
            device_id={"dp": towards[way]},
            device_id_type=MESH,
        )

    def sum_copy(way, short, s, k):
        if s:
            source = came[k].at[way, 2 * (s - 1) + short]
        else:
            source = raw[k].at[way, short] if k or short else begins(way, short, k)
        return send(way, short, s, k, source, came[k].at[way, 2 * s + short])

    for way in range(2):
        sum_copy(way, 0, 0, 0).start()
    for k in range(3):
        all_of_it(raw[k] if k else raw[k].at[:, 1], load_sem.at[k])
        for short in range(k == 0, 2):
            for way in range(2):
                sum_copy(way, short, 0, k).start()
        rest[k].start()
    for copy in owns:
        copy.start()

    squares = jnp.zeros((8, 128), jnp.float32)
    waited = set()
    for s in range(half):
        for k in range(3):
            for short in range(2):
                for way in range(2):
                    here = hops[short] - 1 - s
                    if here < 0:
                        continue
                    layer = layers[way][short]
                    mine = came[k].at[way, 2 * s + short]
                    sum_copy(way, short, s, k).wait_recv()
                    if k not in waited:
                        waited.add(k)
                        rest[k].wait()
                    term = block(held[k], layer, at(sign(way, here)), k)
                    if here > 0:

                        @pl.loop(0, rows[k] // TILE)
                        def _(t):
                            tile = pl.ds(pl.multiple_of(t * TILE, TILE), TILE)
                            mine[tile] = (mine[tile].astype(jnp.float32) + term[tile].astype(jnp.float32)).astype(jnp.bfloat16)

                        sum_copy(way, short, s + 1, k).start()
                    elif not short:
                        other, to = came[k].at[1 - way, 2 * (s - 1) + 1], total[k].at[layer]

                        def add(t, squares):
                            tile = pl.ds(pl.multiple_of(t * TILE, TILE), TILE)
                            g = term[tile].astype(jnp.float32) + mine[tile].astype(jnp.float32) + other[tile].astype(jnp.float32)
                            g = g.astype(jnp.bfloat16)
                            to[tile] = g
                            g = g.astype(jnp.float32)
                            g = g * g
                            for i in range(TILE // 8):
                                for c in range(g.shape[1] // 128):
                                    squares = squares + g[8 * i : 8 * i + 8, 128 * c : 128 * c + 128]
                            return squares

                        squares = lax.fori_loop(0, rows[k] // TILE, add, squares)

    def part_copy(away, sender):
        ref = parts.at[pl.ds(sender, 1)]
        return pltpu.make_async_remote_copy(
            src_ref=ref,
            dst_ref=ref,
            send_sem=part_sem.at[0],
            recv_sem=part_sem.at[1],
            device_id={"dp": at(away)},
            device_id_type=MESH,
        )

    parts[pl.ds(me, 1)] = jnp.sum(squares, axis=0, keepdims=True)
    for away in sorted(range(1, n), key=lambda away: -min(away, n - away)):
        part_copy(away, me).start()
    for copy in owns:
        copy.wait()
    for way in range(2):
        for k in range(3):
            all_of_it(came[k].at[way], send_sem.at[way, k])
    others = parts.at[pl.ds(0, n - 1)]
    for i in range(2):
        all_of_it(others, part_sem.at[i])
    factor = jnp.minimum(1.0, 0.5 * lax.rsqrt(jnp.sum(parts[...], keepdims=True) / count + 1e-30))

    gather = Gather(n, towards, layers, hops, send_sem, recv_sem)
    last = len(weights) - 1
    for k in range(3):
        for layer in range(2):
            to = w_out[k].at[layer] if k == last else block(w_out[k], layer, me, k)


            @pl.loop(0, rows[k] // TILE)
            def _(t):
                tile = pl.ds(pl.multiple_of(t * TILE, TILE), TILE)
                g = total[k][layer, tile].astype(jnp.float32) * factor
                w, m, v = adamw(own[k][layer, tile].astype(jnp.float32), m_own[k][layer, tile], v_own[k][layer, tile], g)
                to[tile] = w
                m_out[k][layer, tile] = m
                v_out[k][layer, tile] = v

            if k < last:
                for way in range(2):
                    gather.copy(w_out[k], way, int(layer != way), 0, k, me, rows[k]).start()
    gather.forward([(w_out[k], rows[k], 0, rows[k]) for k in range(last)], [(k, short) for k in range(last) for short in range(2)])
    for way in range(2):
        for k in range(last):
            all_of_it(came[k].at[way], send_sem.at[way, k])


def kernel_of_the_last(n, own, token, out, send_sem, recv_sem, end_sem):
    del token
    me = lax.axis_index("dp")
    towards = (lax.rem(me + 1, n), lax.rem(me + n - 1, n))
    barrier = pltpu.get_barrier_semaphore()
    for peer in towards:
        pl.semaphore_signal(barrier, inc=1, device_id={"dp": peer}, device_id_type=MESH)
    rows = own.shape[1]
    hops = [n // 2, n // 2 - 1]
    edges = [rows // TILE * p // PIECES * TILE for p in range(PIECES + 1)]
    order = [(p, short) for short in range(2) for p in range(PIECES)]

    def copy(way, short, s, p, behind):
        layer, start, size = way if not short else 1 - way, edges[p], edges[p + 1] - edges[p]
        sender = lax.rem(me + (-behind if way == 0 else behind) + n, n)
        to = out.at[layer, pl.ds(pl.multiple_of(sender * rows + start, TILE), size)]
        return pltpu.make_async_remote_copy(
            src_ref=to if s else own.at[layer, pl.ds(start, size)],
            dst_ref=to,
            send_sem=send_sem.at[way],
            recv_sem=end_sem.at[way] if s == hops[short] - 1 else recv_sem.at[way, 2 * s + short, p],
            device_id={"dp": towards[way]},
            device_id_type=MESH,
        )

    pl.semaphore_wait(barrier, 2)
    for p, short in order:
        for way in range(2):
            copy(way, short, 0, p, 0).start()
    first = pl.multiple_of(me * rows, rows)

    @pl.loop(0, rows // TILE)
    def _(t):
        tile = pl.multiple_of(t * TILE, TILE)
        for layer in range(2):
            out[layer, pl.ds(pl.multiple_of(first + tile, TILE), TILE)] = own[layer, pl.ds(tile, TILE)]

    for s in range(hops[0] - 1):
        for p, short in order:
            for way in range(2):
                if s < hops[short] - 1:
                    copy(way, short, s, p, s + 1).wait_recv()
                    copy(way, short, s + 1, p, s + 1).start()
    for way in range(2):
        all_of_it(own, end_sem.at[way])
        all_of_it(out.at[0, pl.ds(0, sum(hops) * rows)], send_sem.at[way])


def flush(count, *refs):
    sem, tokens = refs[-1], refs[2 * count : -1]
    copies = [pltpu.make_async_copy(refs[i], refs[count + i], sem.at[i]) for i in range(count)]
    for copy in copies:
        copy.start()
    for token in tokens:
        token[...] = jnp.zeros_like(token)
    for copy in copies:
        copy.wait()


def flushed(arrays, *tokens):
    count = len(arrays)
    return pl.pallas_call(
        functools.partial(flush, count),
        name="flush",
        out_shape=[*(jax.ShapeDtypeStruct(a.shape, a.dtype) for a in arrays), *tokens],
        in_specs=[pl.BlockSpec(memory_space=pltpu.VMEM)] * count,
        out_specs=[pl.BlockSpec(memory_space=pl.ANY)] * count + [pl.BlockSpec(memory_space=pltpu.VMEM)] * len(tokens),
        scratch_shapes=[pltpu.SemaphoreType.DMA((count,))],
        compiler_params=pltpu.CompilerParams(vmem_limit_bytes=2**20),
    )(*arrays)


def solution(mesh):
    def step(*arrays):
        n = lax.axis_size("dp")
        terms, weights, m, v = (arrays[i : i + 3] for i in (0, 3, 6, 9))
        count = sum(w.size for w in weights)
        shapes = [(w.shape, w.dtype) for w in weights[:-1]] + [(m[-1].shape, weights[-1].dtype)] + [(x.shape, x.dtype) for x in (*m, *v)]
        blocks = [(one.shape[1], one.shape[2]) for one in m]
        half = n // 2
        outs = pl.pallas_call(
            functools.partial(kernel, n, count),
            name="step",
            out_shape=[pltpu.VMEM(s, d) for s, d in shapes],
            in_specs=[pl.BlockSpec(memory_space=pl.ANY)] * 12,
            out_specs=[pl.BlockSpec(memory_space=pltpu.VMEM)] * 9,
            scratch_shapes=[
                *(pltpu.VMEM((2, 2, *b), jnp.bfloat16) for b in blocks),
                *(pltpu.VMEM(w.shape, jnp.bfloat16) for w in weights),
                *(pltpu.VMEM((2, 2 * half - 1, *b), jnp.bfloat16) for b in blocks),
                *(pltpu.VMEM((2, *b), jnp.bfloat16) for b in blocks),
                *(pltpu.VMEM((2, *b), jnp.float32) for b in blocks * 2),
                *(pltpu.VMEM((2, *b), jnp.bfloat16) for b in blocks),
                pltpu.VMEM((n, 128), jnp.float32),
                pltpu.SemaphoreType.DMA((3,)),
                pltpu.SemaphoreType.DMA((3, 3)),
                pltpu.SemaphoreType.DMA((2, 3)),
                pltpu.SemaphoreType.DMA((2, 2 * half - 1, 3)),
                pltpu.SemaphoreType.DMA((2,)),
            ],
            compiler_params=pltpu.CompilerParams(collective_id=0, has_side_effects=True, vmem_limit_bytes=48 * 2**20),
        )(*arrays)
        *whole, own, m0, m1, m2, v0, v1, v2 = outs
        *done, token = flushed([*whole, m0, m1, m2, v0, v1, v2], pltpu.VMEM((8, 128), jnp.float32))
        last = pl.pallas_call(
            functools.partial(kernel_of_the_last, n),
            name="last",
            out_shape=pltpu.VMEM(weights[-1].shape, weights[-1].dtype),
            in_specs=[pl.BlockSpec(memory_space=pltpu.VMEM)] * 2,
            out_specs=pl.BlockSpec(memory_space=pltpu.VMEM),
            scratch_shapes=[
                pltpu.SemaphoreType.DMA((2,)),
                pltpu.SemaphoreType.DMA((2, 2 * half - 3, PIECES)),
                pltpu.SemaphoreType.DMA((2,)),
            ],
            compiler_params=pltpu.CompilerParams(collective_id=1, has_side_effects=True, vmem_limit_bytes=2**20),
        )(own, token)
        return (*done[: len(whole)], *flushed([last]), *done[len(whole) :])

    all_of, cut = P(None, None, None), P(None, "dp", None)
    return jax.shard_map(
        step,
        mesh=mesh,
        in_specs=(P(("rep", "dp"), None, None, None),) * 3 + (all_of,) * 3 + (cut,) * 6,
        out_specs=(P("rep", None, None),) * 3 + (P("rep", "dp", None),) * 6,
        check_vma=False,
    )
```

```python
import functools

import jax
import jax.numpy as jnp
from jax import lax
from jax.experimental import pallas as pl
from jax.experimental.pallas import tpu as pltpu
from jax.sharding import PartitionSpec as P

MESH = pl.DeviceIdType.MESH
TILE = 16
PIECES = 2
LATER = 9500


def adamw(w, m, v, g):
    m = 0.9 * m + 0.1 * g
    v = 0.95 * v + 0.05 * g * g
    step = m * lax.rsqrt(v + 1e-8) + 0.1 * w
    return (w - 0.02 * step).astype(jnp.bfloat16), m, v


def all_of_it(ref, sem):
    pltpu.make_async_copy(ref, ref, sem).wait()


class Gather:
    def __init__(self, n, towards, layers, hops, send_sem, recv_sem):
        self.n, self.towards, self.layers, self.hops = n, towards, layers, hops
        self.send_sem, self.recv_sem = send_sem, recv_sem
        self.me = lax.axis_index("dp")

    def behind(self, way, s):
        return lax.rem(self.me + (-s if way == 0 else s) + self.n, self.n)

    def copy(self, ref, way, short, s, p, sender, rows, start=0, size=None, source=None):
        to = ref.at[self.layers[way][short], pl.ds(pl.multiple_of(sender * rows + start, TILE), size or rows)]
        return pltpu.make_async_remote_copy(
            src_ref=to if source is None else source,
            dst_ref=to,
            send_sem=self.send_sem.at[way, p],
            recv_sem=self.recv_sem.at[way, 2 * s + short, p],
            device_id={"dp": self.towards[way]},
            device_id_type=MESH,
        )

    def forward(self, pieces, order):
        for s in range(self.hops[0]):
            for p, short in order:
                ref, rows, start, size = pieces[p]
                for way in range(2):
                    if s >= self.hops[short]:
                        continue

                    def copy(step, behind):
                        return self.copy(ref, way, short, step, p, self.behind(way, behind), rows, start, size)

                    copy(s, s + 1).wait_recv()
                    if s + 1 < self.hops[short]:
                        copy(s + 1, s + 1).start()


def kernel(n, count, *refs):
    terms, weights, m_in, v_in = (refs[i : i + 3] for i in (0, 3, 6, 9))
    w_out, m_out, v_out = (refs[i : i + 3] for i in (12, 15, 18))
    raw, held, came, own, m_own, v_own, total = (refs[i : i + 3] for i in range(21, 42, 3))
    parts, load_sem, own_sem, send_sem, recv_sem, part_sem = refs[42:]
    me = lax.axis_index("dp")
    rows = [m.shape[1] for m in m_in]
    half = n // 2

    def at(away):
        return lax.rem(me + away + n, n)

    def sign(way, away):
        return away if way == 0 else -away

    def block(ref, layer, who, k):
        return ref.at[layer, pl.ds(pl.multiple_of(who * rows[k], rows[k]), rows[k])]

    towards = (at(1), at(-1))
    layers = [[way, 1 - way] for way in range(2)]
    hops = [half, half - 1]

    barrier = pltpu.get_barrier_semaphore()
    for peer in towards:
        pl.semaphore_signal(barrier, inc=1, device_id={"dp": peer}, device_id_type=MESH)

    def begins(way, short, k):
        return block(terms[k].at[0], layers[way][short], at(sign(way, hops[short])), k)

    rest = [pltpu.make_async_copy(terms[k].at[0], held[k], load_sem.at[k]) for k in range(3)]
    owns = [
        pltpu.make_async_copy(source, to, own_sem.at[i, k])
        for k in range(3)
        for i, (source, to) in enumerate(
            [(weights[k].at[:, pl.ds(pl.multiple_of(me * rows[k], rows[k]), rows[k])], own[k]), (m_in[k], m_own[k]), (v_in[k], v_own[k])]
        )
    ]
    for k in range(3):
        for short in range(k == 0, 2):
            for way in range(2):
                pltpu.make_async_copy(begins(way, short, k), raw[k].at[way, short], load_sem.at[k]).start()
    pl.semaphore_wait(barrier, 2)

    @pl.when(lax.rem(lax.axis_index("rep"), 2) == 0)
    def _():
        pl.delay(LATER)

    def send(way, short, s, k, source, to):
        return pltpu.make_async_remote_copy(
            src_ref=source,
            dst_ref=to,
            send_sem=send_sem.at[way, k],
            recv_sem=recv_sem.at[way, 2 * s + short, k],
            device_id={"dp": towards[way]},
            device_id_type=MESH,
        )

    def sum_copy(way, short, s, k):
        if s:
            source = came[k].at[way, 2 * (s - 1) + short]
        else:
            source = raw[k].at[way, short] if k or short else begins(way, short, k)
        return send(way, short, s, k, source, came[k].at[way, 2 * s + short])

    for way in range(2):
        sum_copy(way, 0, 0, 0).start()
    for k in range(3):
        all_of_it(raw[k] if k else raw[k].at[:, 1], load_sem.at[k])
        for short in range(k == 0, 2):
            for way in range(2):
                sum_copy(way, short, 0, k).start()
        rest[k].start()
    for copy in owns:
        copy.start()

    squares = jnp.zeros((8, 128), jnp.float32)
    waited = set()
    for s in range(half):
        for k in range(3):
            for short in range(2):
                for way in range(2):
                    here = hops[short] - 1 - s
                    if here < 0:
                        continue
                    layer = layers[way][short]
                    mine = came[k].at[way, 2 * s + short]
                    sum_copy(way, short, s, k).wait_recv()
                    if k not in waited:
                        waited.add(k)
                        rest[k].wait()
                    term = block(held[k], layer, at(sign(way, here)), k)
                    if here > 0:

                        @pl.loop(0, rows[k] // TILE)
                        def _(t):
                            tile = pl.ds(pl.multiple_of(t * TILE, TILE), TILE)
                            mine[tile] = (mine[tile].astype(jnp.float32) + term[tile].astype(jnp.float32)).astype(jnp.bfloat16)

                        sum_copy(way, short, s + 1, k).start()
                    elif not short:
                        other, to = came[k].at[1 - way, 2 * (s - 1) + 1], total[k].at[layer]

                        def add(t, squares):
                            tile = pl.ds(pl.multiple_of(t * TILE, TILE), TILE)
                            g = term[tile].astype(jnp.float32) + mine[tile].astype(jnp.float32) + other[tile].astype(jnp.float32)
                            g = g.astype(jnp.bfloat16)
                            to[tile] = g
                            g = g.astype(jnp.float32)
                            g = g * g
                            for i in range(TILE // 8):
                                for c in range(g.shape[1] // 128):
                                    squares = squares + g[8 * i : 8 * i + 8, 128 * c : 128 * c + 128]
                            return squares

                        squares = lax.fori_loop(0, rows[k] // TILE, add, squares)

    def part_copy(away, sender):
        ref = parts.at[pl.ds(sender, 1)]
        return pltpu.make_async_remote_copy(
            src_ref=ref,
            dst_ref=ref,
            send_sem=part_sem.at[0],
            recv_sem=part_sem.at[1],
            device_id={"dp": at(away)},
            device_id_type=MESH,
        )

    parts[pl.ds(me, 1)] = jnp.sum(squares, axis=0, keepdims=True)
    for away in sorted(range(1, n), key=lambda away: -min(away, n - away)):
        part_copy(away, me).start()
    for copy in owns:
        copy.wait()
    for way in range(2):
        for k in range(3):
            all_of_it(came[k].at[way], send_sem.at[way, k])
    others = parts.at[pl.ds(0, n - 1)]
    for i in range(2):
        all_of_it(others, part_sem.at[i])
    factor = jnp.minimum(1.0, 0.5 * lax.rsqrt(jnp.sum(parts[...], keepdims=True) / count + 1e-30))

    gather = Gather(n, towards, layers, hops, send_sem, recv_sem)
    last = len(weights) - 1
    for k in range(3):
        for layer in range(2):
            to = w_out[k].at[layer] if k == last else block(w_out[k], layer, me, k)


            @pl.loop(0, rows[k] // TILE)
            def _(t):
                tile = pl.ds(pl.multiple_of(t * TILE, TILE), TILE)
                g = total[k][layer, tile].astype(jnp.float32) * factor
                w, m, v = adamw(own[k][layer, tile].astype(jnp.float32), m_own[k][layer, tile], v_own[k][layer, tile], g)
                to[tile] = w
                m_out[k][layer, tile] = m
                v_out[k][layer, tile] = v

            if k < last:
                for way in range(2):
                    gather.copy(w_out[k], way, int(layer != way), 0, k, me, rows[k]).start()
    gather.forward([(w_out[k], rows[k], 0, rows[k]) for k in range(last)], [(k, short) for k in range(last) for short in range(2)])
    for way in range(2):
        for k in range(last):
            all_of_it(came[k].at[way], send_sem.at[way, k])


def kernel_of_the_last(n, own, token, out, send_sem, recv_sem, end_sem):
    del token
    me = lax.axis_index("dp")
    towards = (lax.rem(me + 1, n), lax.rem(me + n - 1, n))
    barrier = pltpu.get_barrier_semaphore()
    for peer in towards:
        pl.semaphore_signal(barrier, inc=1, device_id={"dp": peer}, device_id_type=MESH)
    rows = own.shape[1]
    hops = [n // 2, n // 2 - 1]
    edges = [rows // TILE * p // PIECES * TILE for p in range(PIECES + 1)]
    order = [(p, short) for short in range(2) for p in range(PIECES)]

    def copy(way, short, s, p, behind):
        layer, start, size = way if not short else 1 - way, edges[p], edges[p + 1] - edges[p]
        sender = lax.rem(me + (-behind if way == 0 else behind) + n, n)
        to = out.at[layer, pl.ds(pl.multiple_of(sender * rows + start, TILE), size)]
        return pltpu.make_async_remote_copy(
            src_ref=to if s else own.at[layer, pl.ds(start, size)],
            dst_ref=to,
            send_sem=send_sem.at[way],
            recv_sem=end_sem.at[way] if s == hops[short] - 1 else recv_sem.at[way, 2 * s + short, p],
            device_id={"dp": towards[way]},
            device_id_type=MESH,
        )

    pl.semaphore_wait(barrier, 2)
    for p, short in order:
        for way in range(2):
            copy(way, short, 0, p, 0).start()
    first = pl.multiple_of(me * rows, rows)

    @pl.loop(0, rows // TILE)
    def _(t):
        tile = pl.multiple_of(t * TILE, TILE)
        for layer in range(2):
            out[layer, pl.ds(pl.multiple_of(first + tile, TILE), TILE)] = own[layer, pl.ds(tile, TILE)]

    for s in range(hops[0] - 1):
        for p, short in order:
            for way in range(2):
                if s < hops[short] - 1:
                    copy(way, short, s, p, s + 1).wait_recv()
                    copy(way, short, s + 1, p, s + 1).start()
    for way in range(2):
        all_of_it(own, end_sem.at[way])
        all_of_it(out.at[0, pl.ds(0, sum(hops) * rows)], send_sem.at[way])


def flush(count, *refs):
    sem, tokens = refs[-1], refs[2 * count : -1]
    copies = [pltpu.make_async_copy(refs[i], refs[count + i], sem.at[i]) for i in range(count)]
    for copy in copies:
        copy.start()
    for token in tokens:
        token[...] = jnp.zeros_like(token)
    for copy in copies:
        copy.wait()


def flushed(arrays, *tokens):
    count = len(arrays)
    return pl.pallas_call(
        functools.partial(flush, count),
        name="flush",
        out_shape=[*(jax.ShapeDtypeStruct(a.shape, a.dtype) for a in arrays), *tokens],
        in_specs=[pl.BlockSpec(memory_space=pltpu.VMEM)] * count,
        out_specs=[pl.BlockSpec(memory_space=pl.ANY)] * count + [pl.BlockSpec(memory_space=pltpu.VMEM)] * len(tokens),
        scratch_shapes=[pltpu.SemaphoreType.DMA((count,))],
        compiler_params=pltpu.CompilerParams(vmem_limit_bytes=2**20),
    )(*arrays)


def solution(mesh):
    def step(*arrays):
        n = lax.axis_size("dp")
        terms, weights, m, v = (arrays[i : i + 3] for i in (0, 3, 6, 9))
        count = sum(w.size for w in weights)
        shapes = [(w.shape, w.dtype) for w in weights[:-1]] + [(m[-1].shape, weights[-1].dtype)] + [(x.shape, x.dtype) for x in (*m, *v)]
        blocks = [(one.shape[1], one.shape[2]) for one in m]
        half = n // 2
        outs = pl.pallas_call(
            functools.partial(kernel, n, count),
            name="step",
            out_shape=[pltpu.VMEM(s, d) for s, d in shapes],
            in_specs=[pl.BlockSpec(memory_space=pl.ANY)] * 12,
            out_specs=[pl.BlockSpec(memory_space=pltpu.VMEM)] * 9,
            scratch_shapes=[
                *(pltpu.VMEM((2, 2, *b), jnp.bfloat16) for b in blocks),
                *(pltpu.VMEM(w.shape, jnp.bfloat16) for w in weights),
                *(pltpu.VMEM((2, 2 * half - 1, *b), jnp.bfloat16) for b in blocks),
                *(pltpu.VMEM((2, *b), jnp.bfloat16) for b in blocks),
                *(pltpu.VMEM((2, *b), jnp.float32) for b in blocks * 2),
                *(pltpu.VMEM((2, *b), jnp.bfloat16) for b in blocks),
                pltpu.VMEM((n, 128), jnp.float32),
                pltpu.SemaphoreType.DMA((3,)),
                pltpu.SemaphoreType.DMA((3, 3)),
                pltpu.SemaphoreType.DMA((2, 3)),
                pltpu.SemaphoreType.DMA((2, 2 * half - 1, 3)),
                pltpu.SemaphoreType.DMA((2,)),
            ],
            compiler_params=pltpu.CompilerParams(collective_id=0, has_side_effects=True, vmem_limit_bytes=48 * 2**20),
        )(*arrays)
        *whole, own, m0, m1, m2, v0, v1, v2 = outs
        *done, token = flushed([*whole, m0, m1, m2, v0, v1, v2], pltpu.VMEM((8, 128), jnp.float32))
        last = pl.pallas_call(
            functools.partial(kernel_of_the_last, n),
            name="last",
            out_shape=pltpu.VMEM(weights[-1].shape, weights[-1].dtype),
            in_specs=[pl.BlockSpec(memory_space=pltpu.VMEM)] * 2,
            out_specs=pl.BlockSpec(memory_space=pltpu.VMEM),
            scratch_shapes=[
                pltpu.SemaphoreType.DMA((2,)),
                pltpu.SemaphoreType.DMA((2, 2 * half - 3, PIECES)),
                pltpu.SemaphoreType.DMA((2,)),
            ],
            compiler_params=pltpu.CompilerParams(collective_id=1, has_side_effects=True, vmem_limit_bytes=2**20),
        )(own, token)
        return (*done[: len(whole)], *flushed([last]), *done[len(whole) :])

    all_of, cut = P(None, None, None), P(None, "dp", None)
    return jax.shard_map(
        step,
        mesh=mesh,
        in_specs=(P(("rep", "dp"), None, None, None),) * 3 + (all_of,) * 3 + (cut,) * 6,
        out_specs=(P("rep", None, None),) * 3 + (P("rep", "dp", None),) * 6,
        check_vma=False,
    )
```
